128 devices in a mesh: space: 128 (over x, y, z, core).
Axes of the slice: x: 4, y: 4, z: 4, core: 2. Of those that a mesh axis runs over, the one named last changes fastest.
Arguments:
- positions: float32 [3, 524288], P(None, 'space'), may hold values from 1 to 512, as said below
- velocity: float32 [3, 524288], P(None, 'space'), may hold values from -5 to 5
- deformation: float32 [9, 524288], P(None, 'space'), may hold values from -0.6 to 1.6
- affine: float32 [9, 524288], P(None, 'space'), may hold values from -3 to 3
- particle_mass: float32 [524288], P('space'), may hold values from 0.05 to 0.3
- volume: float32 [524288], P('space'), may hold values from 0.06 to 0.25
- bin_block: int32 [1024], P('space'), may hold values from 0 to 255
- live_count: int32 [128], P('space'), may hold values from 2 to 4, as said below
Outputs:
- displacement: float32 [3, 524288], P(None, 'space')
- new_velocity: float32 [3, 524288], P(None, 'space')
- new_deformation: float32 [9, 524288], P(None, 'space')
- new_affine: float32 [9, 524288], P(None, 'space')
The draws below stay inside these ranges and needn't reach their ends.
Inputs may be any that keep to these rules, and one draw needn't show every extreme that they name: `positions`: each particle lies inside its bin's block: 4 d + 1 to 4 d + 4 along the first dimension for the bins of device d, 4 (bin_block // 16) + 1 to 4 (bin_block // 16) + 4 along the second, 4 (bin_block % 16) + 1 to 4 (bin_block % 16) + 4 along the third. The live bins of device d are its first live_count[d] slots; devices 2 k and 2 k + 1 hold at most 6 live bins together, and some such pair holds exactly 6 in every draw.
All inputs are finite; a program needn't handle non-finite values.
Results may differ from the reference program's by a relative error of at most 0.0003.
Values sent between devices are 32-bit elements; how exact they have to be, the bound alone decides.
A program may use at most 128 MiB of HBM per device.

```python
import math
import jax
import jax.numpy as jnp
from jax import lax

PPB = 512
BIN_CAP = 8
BY = 16
BZ = 16
STEPS = 3
BINS = 1024
NGY = 66
NGZ = 66
N_SPACE = 128


def shared_blocks(key):
    return jax.random.randint(jax.random.fold_in(key, 7), (BINS,), 0, BY * BZ, dtype=jnp.int32)


def draw_bin_block(key, part):
    return shared_blocks(key)


def draw_positions(key, part):
    blocks = shared_blocks(key)
    home_devices = jnp.arange(BINS, dtype=jnp.int32) // BIN_CAP
    anchor = jnp.stack([4 * home_devices, 4 * (blocks // BZ), 4 * (blocks % BZ)]).astype(jnp.float32)
    fraction = jax.random.uniform(jax.random.fold_in(key, 8), (3, BINS, PPB), jnp.float32)
    return (anchor[:, :, None] + 1.0 + 3.0 * fraction).reshape(3, BINS * PPB)


def draw_deformation(key, part):
    identity = jnp.eye(3, dtype=jnp.float32).reshape(9, 1)
    noise_key = jax.random.fold_in(key, 9)
    noise = jnp.clip(0.15 * jax.random.normal(noise_key, (9, BINS * PPB), jnp.float32), -0.6, 0.6)
    return identity + noise


def draw_live_count(key, part):
    pair_total = N_SPACE // 2
    keys = [jax.random.fold_in(key, 20 + number) for number in range(5)]
    totals = jax.random.randint(keys[0], (pair_total,), 4, BIN_CAP - 1, dtype=jnp.int32)
    totals = totals.at[0].set(BIN_CAP - 2)
    lower_share = jnp.maximum(2, totals - (BIN_CAP - 4))
    upper_share = jnp.minimum(totals - 2, BIN_CAP - 4)
    share_span = upper_share - lower_share + 1
    random_picks = [jax.random.randint(keys[1 + number], (pair_total,), 0, 1 << 20, dtype=jnp.int32) % share_span for number in range(3)]
    smaller = lower_share + jnp.minimum(jnp.minimum(random_picks[0], random_picks[1]), random_picks[2])
    larger_share = totals - smaller
    flip_order = jax.random.randint(keys[4], (pair_total,), 0, 2, dtype=jnp.int32)
    first_count = jnp.where(flip_order == 1, smaller, larger_share)
    second_count = totals - first_count
    return jnp.stack([first_count, second_count], axis=1).reshape(N_SPACE).astype(jnp.int32)


def steps_of(key, dims, shards, low, top_value):
    loudness, own = 1.0, jax.random.fold_in(key, 6)
    for dim, parts in shards:
        draws = jnp.exp(jax.random.uniform(jax.random.fold_in(own, dim), (parts,), jnp.float32, low / len(shards), top_value / len(shards)))
        loudness = loudness * jnp.repeat(draws, dims[dim] // parts).reshape([-1 if axis == dim else 1 for axis in range(len(dims))])
    return loudness


def bell_draw(rng, dims, width, bound, shards=(), kind=jnp.bfloat16):
    values = width * jax.random.normal(rng, dims, jnp.float32)
    if shards:
        values = values * steps_of(rng, dims, shards, -0.22, 0.18)
    return jnp.clip(values, -bound, bound).astype(kind)


def setup_inputs(seed: int = 0) -> dict:
    splits = jax.random.split(jax.random.key(seed), 9)
    positions = draw_positions(jax.random.fold_in(splits[8], 71), 0)
    velocity = bell_draw(splits[1], (3, BINS * PPB), 1.0, 5.0, ((1, 128),), jnp.float32)
    deformation = draw_deformation(jax.random.fold_in(splits[8], 71), 0)
    affine = bell_draw(splits[3], (9, BINS * PPB), 0.5, 3.0, ((1, 128),), jnp.float32)
    particle_mass = jnp.clip(jnp.exp(math.log(0.3) - 1.7917595 * jax.random.uniform(splits[4], (BINS * PPB,), jnp.float32) ** steps_of(splits[4], (BINS * PPB,), ((0, 128),), -0.2, 0.2)), 0.05, 0.3)
    volume = jnp.clip(jnp.exp(math.log(0.25) - 1.4271164 * jax.random.uniform(splits[5], (BINS * PPB,), jnp.float32) ** steps_of(splits[5], (BINS * PPB,), ((0, 128),), -0.2, 0.2)), 0.06, 0.25)
    bin_block = draw_bin_block(jax.random.fold_in(splits[8], 71), 0)
    live_count = draw_live_count(jax.random.fold_in(splits[8], 71), 0)
    return dict(positions=positions, velocity=velocity, deformation=deformation, affine=affine, particle_mass=particle_mass, volume=volume, bin_block=bin_block, live_count=live_count)


mu_shear = 4.0
lame_first = 6.0
courant = 0.15
sound_speed = 3.7416573867739413
mass_floor = 0.05
gravity_x = 3.0
gravity_z = -9.0
highest = lax.Precision.HIGHEST

def spline(distance):
    magnitude = jnp.abs(distance)
    inner_part = 0.75 - magnitude * magnitude
    outer_part = 0.5 * (1.5 - magnitude) * (1.5 - magnitude)
    return jnp.where(magnitude < 0.5, inner_part, jnp.where(magnitude < 1.5, outer_part, 0.0 * magnitude))

def node_coords():
    numbers = jnp.arange(216, dtype=jnp.int32)
    return jnp.stack([numbers // 36, numbers // 6 % 6, numbers % 6]).astype(jnp.float32)

def spline_weights(local_coords):
    offsets = jnp.arange(6, dtype=jnp.int32).astype(jnp.float32)
    per_axis = [spline(offsets[None, :, None] - local_coords[number][:, None, :]) for number in range(3)]
    weight_table = per_axis[0][:, :, None, None, :] * per_axis[1][:, None, :, None, :] * per_axis[2][:, None, None, :, :]
    return weight_table.reshape(local_coords.shape[1], 216, local_coords.shape[2])

def block_anchor(home_devices, blocks):
    return jnp.stack([4 * home_devices, 4 * (blocks // BZ), 4 * (blocks % BZ)]).astype(jnp.float32)

def selectors(starts, node_total):
    columns = jnp.arange(node_total, dtype=jnp.int32)
    offsets = jnp.arange(6, dtype=jnp.int32)
    return (columns[None, None, :] == 4 * starts[:, None, None] + offsets[None, :, None]).astype(jnp.float32)

def plane_selector(select_y, select_z):
    joined = select_y[:, :, None, :, None] * select_z[:, None, :, None, :]
    return joined.reshape(select_y.shape[0], 36, select_y.shape[2] * select_z.shape[2])

def kirchhoff(deform):
    entries = [deform[number] for number in range(9)]
    determinant = entries[0] * (entries[4] * entries[8] - entries[5] * entries[7]) - entries[1] * (entries[3] * entries[8] - entries[5] * entries[6]) + entries[2] * (entries[3] * entries[7] - entries[4] * entries[6])
    pressure_term = lame_first * (determinant - 1.0) * determinant
    stress = []
    for outer_index in range(3):
        for inner_index in range(3):
            product = entries[3 * outer_index] * entries[3 * inner_index] + entries[3 * outer_index + 1] * entries[3 * inner_index + 1] + entries[3 * outer_index + 2] * entries[3 * inner_index + 2]
            if outer_index == inner_index:
                stress.append(mu_shear * (product - 1.0) + pressure_term)
            else:
                stress.append(mu_shear * product)
    return stress

def particle_to_grid(working, local_coords, weight_table, time_step):
    stress = kirchhoff(working[6:15])
    masses = working[24]
    volumes = working[25]
    affine_term = [masses * working[15 + number] - 4.0 * time_step * volumes * stress[number] for number in range(9)]
    momentum = []
    for outer_index in range(3):
        shifted = masses * working[3 + outer_index]
        for inner_index in range(3):
            shifted = shifted - affine_term[3 * outer_index + inner_index] * local_coords[inner_index]
        momentum.append(shifted)
    quantities = jnp.stack([masses] + momentum + affine_term)
    summed = jnp.einsum('cbp,bnp->bcn', quantities, weight_table, precision=highest)
    nodes = node_coords()
    moments = []
    for outer_index in range(3):
        total_moment = summed[:, 1 + outer_index]
        for inner_index in range(3):
            total_moment = total_moment + summed[:, 4 + 3 * outer_index + inner_index] * nodes[inner_index][None, :]
        moments.append(total_moment)
    return jnp.stack([summed[:, 0]] + moments, axis=1)

def scatter_tiles(node_tiles, select_y, select_z):
    select_plane = plane_selector(select_y, select_z)
    shaped = node_tiles.reshape(node_tiles.shape[0], 24, 36)
    spread = jnp.einsum('bqn,bnm->qm', shaped, select_plane, precision=highest)
    return spread.reshape(4, 6, select_y.shape[2], select_z.shape[2])

def tile_velocities(slab_velocity, select_y, select_z):
    select_plane = plane_selector(select_y, select_z)
    flat = slab_velocity.reshape(18, select_plane.shape[2])
    gathered = jnp.einsum('qm,bnm->bqn', flat, select_plane, precision=highest)
    return gathered.reshape(gathered.shape[0], 3, 216)

def grid_velocity(owned_planes, device, time_step, plane_total):
    node_mass = jnp.maximum(owned_planes[0], mass_floor)
    planes = 4 * device + jnp.arange(4, dtype=jnp.int32)
    column_y = jnp.arange(owned_planes.shape[2], dtype=jnp.int32)
    column_z = jnp.arange(owned_planes.shape[3], dtype=jnp.int32)
    along_x = owned_planes[1] / node_mass + time_step * gravity_x
    along_y = owned_planes[2] / node_mass
    along_z = owned_planes[3] / node_mass + time_step * gravity_z
    along_x = jnp.where((planes < 2)[:, None, None], jnp.maximum(along_x, 0.0), along_x)
    along_x = jnp.where((planes >= plane_total - 2)[:, None, None], jnp.minimum(along_x, 0.0), along_x)
    along_y = jnp.where((column_y < 2)[None, :, None], jnp.maximum(along_y, 0.0), along_y)
    along_y = jnp.where((column_y >= owned_planes.shape[2] - 2)[None, :, None], jnp.minimum(along_y, 0.0), along_y)
    along_z = jnp.where((column_z < 2)[None, None, :], jnp.maximum(along_z, 0.0), along_z)
    along_z = jnp.where((column_z >= owned_planes.shape[3] - 2)[None, None, :], jnp.minimum(along_z, 0.0), along_z)
    return jnp.stack([along_x, along_y, along_z])

def grid_to_particle(working, local_coords, weight_table, velocity_tiles, time_step):
    nodes = node_coords()
    node_terms = [velocity_tiles[:, number] for number in range(3)]
    for outer_index in range(3):
        for inner_index in range(3):
            node_terms.append(velocity_tiles[:, outer_index] * nodes[inner_index][None, :])
    stacked = jnp.stack(node_terms, axis=1)
    interpolated = jnp.einsum('bcn,bnp->cbp', stacked, weight_table, precision=highest)
    new_motion = interpolated[0:3]
    affine_new = []
    for outer_index in range(3):
        for inner_index in range(3):
            affine_new.append(4.0 * (interpolated[3 + 3 * outer_index + inner_index] - new_motion[outer_index] * local_coords[inner_index]))
    deform = working[6:15]
    deform_new = []
    for outer_index in range(3):
        for inner_index in range(3):
            updated = deform[3 * outer_index + inner_index]
            for middle_index in range(3):
                updated = updated + time_step * affine_new[3 * outer_index + middle_index] * deform[3 * middle_index + inner_index]
            deform_new.append(updated)
    moved = working[0:3] + time_step * new_motion
    travelled = working[26:29] + time_step * new_motion
    return jnp.concatenate([moved, new_motion, jnp.stack(deform_new), jnp.stack(affine_new), working[24:26], travelled])

def prepare(working, device, device_blocks):
    home_devices = jnp.zeros_like(device_blocks) + device
    anchor = block_anchor(home_devices, device_blocks)
    local_coords = working[0:3] - anchor[:, :, None]
    return (local_coords, spline_weights(local_coords))

def reference(positions, velocity, deformation, affine, particle_mass, volume, bin_block, live_count):
    slot_ids = jnp.arange(BIN_CAP, dtype=jnp.int32)
    live_slots = (slot_ids[None, :] < live_count[:, None]).astype(jnp.float32)
    masked_mass = particle_mass.reshape(N_SPACE, BIN_CAP, PPB) * live_slots[:, :, None]
    masked_volume = volume.reshape(N_SPACE, BIN_CAP, PPB) * live_slots[:, :, None]
    grouped = jnp.concatenate([positions, velocity, deformation, affine]).reshape(24, N_SPACE, BIN_CAP, PPB)
    travelled = jnp.zeros((3, N_SPACE, BIN_CAP, PPB), jnp.float32)
    particle_state = jnp.concatenate([grouped, masked_mass[None], masked_volume[None], travelled]).transpose(1, 0, 2, 3)
    blocks = bin_block.reshape(N_SPACE, BIN_CAP)
    devices = jnp.arange(N_SPACE, dtype=jnp.int32)
    plane_total = 4 * N_SPACE
    for iteration in range(STEPS):
        speed_squared = jnp.where(particle_state[:, 24] > 0.0, lax.optimization_barrier(jnp.sum(particle_state[:, 3:6] * particle_state[:, 3:6], axis=1)), 0.0)
        time_step = courant / (jnp.sqrt(jnp.max(speed_squared)) + sound_speed)

        def partial_of(inputs):
            device, working, device_blocks = inputs
            local_coords, weight_table = prepare(working, device, device_blocks)
            node_tiles = particle_to_grid(working, local_coords, weight_table, time_step)
            return scatter_tiles(node_tiles, selectors(device_blocks // BZ, NGY), selectors(device_blocks % BZ, NGZ))
        partials = lax.map(partial_of, (devices, particle_state, blocks))
        incoming = jnp.concatenate([jnp.zeros((1, 4, 2, NGY, NGZ), jnp.float32), partials[:-1, :, 4:6]])
        owned_planes = jnp.concatenate([partials[:, :, 0:2] + incoming, partials[:, :, 2:4]], axis=2)
        motion = jax.vmap(grid_velocity, in_axes=(0, 0, None, None))(owned_planes, devices, time_step, plane_total)
        ghost_planes = jnp.concatenate([motion[1:, :, 0:2], jnp.zeros((1, 3, 2, NGY, NGZ), jnp.float32)])
        slab_velocity = jnp.concatenate([motion, ghost_planes], axis=2)

        def update_of(inputs):
            device, working, device_blocks, device_velocity = inputs
            local_coords, weight_table = prepare(working, device, device_blocks)
            velocity_tiles = tile_velocities(device_velocity, selectors(device_blocks // BZ, NGY), selectors(device_blocks % BZ, NGZ))
            return grid_to_particle(working, local_coords, weight_table, velocity_tiles, time_step)
        particle_state = lax.map(update_of, (devices, particle_state, blocks, slab_velocity))
    finished = jnp.concatenate([particle_state[:, 26:29], particle_state[:, 3:24]], axis=1) * live_slots[:, None, :, None]
    flattened = finished.transpose(1, 0, 2, 3).reshape(24, BINS * PPB)
    return (flattened[0:3], flattened[3:6], flattened[6:15], flattened[15:24])
```

```python
import functools
import itertools

import jax
import jax.numpy as jnp
from jax import lax
from jax.experimental import pallas as pl
from jax.experimental.pallas import tpu as pltpu
from jax.sharding import PartitionSpec as P

STEPS = 3
LIVE = 4
PPB = 512
PARTICLES = LIVE * PPB
TILES = PARTICLES // 128
BIG = 3.4028235e38
FAR = 1e18
MESH = pl.DeviceIdType.MESH
F32 = jnp.float32
BF16 = jnp.bfloat16

mu_shear = 4.0
lame_first = 6.0
courant = 0.15
sound_speed = 3.7416573867739413
mass_floor = 0.05
gravity_x = 3.0
gravity_z = -9.0


def ring_distance(step):
    return min(step, 4 - step)


def peer_offsets():
    offsets = [o for o in itertools.product(range(4), range(4), range(4), range(2)) if any(o)]
    offsets.sort(key=lambda o: -(sum(ring_distance(c) for c in o[:3]) + 0.1 * o[3]))
    return offsets


def peer_at(me, offset):
    x, y, z, core = me // 32, me // 8 % 4, me // 2 % 4, me % 2
    x, y, z = (x + offset[0]) % 4, (y + offset[1]) % 4, (z + offset[2]) % 4
    return ((x * 4 + y) * 4 + z) * 2 + (core + offset[3]) % 2


PEERS = peer_offsets()


def halves(value):
    high = value.astype(BF16)
    return high, (value - high.astype(F32)).astype(BF16)


def spline(distance):
    magnitude = jnp.abs(distance)
    inner_part = 0.75 - magnitude * magnitude
    outer_part = 0.5 * (1.5 - magnitude) * (1.5 - magnitude)
    return jnp.where(magnitude < 0.5, inner_part, jnp.where(magnitude < 1.5, outer_part, 0.0))


def kirchhoff(f):
    determinant = (
        f[0] * (f[4] * f[8] - f[5] * f[7])
        - f[1] * (f[3] * f[8] - f[5] * f[6])
        + f[2] * (f[3] * f[7] - f[4] * f[6])
    )
    pressure = lame_first * (determinant - 1.0) * determinant
    stress = [None] * 9
    for r in range(3):
        for c in range(r, 3):
            product = f[3 * r] * f[3 * c] + f[3 * r + 1] * f[3 * c + 1] + f[3 * r + 2] * f[3 * c + 2]
            value = mu_shear * (product - 1.0) + pressure if r == c else mu_shear * product
            stress[3 * r + c] = stress[3 * c + r] = value
    return stress


def iota(shape, axis):
    return lax.broadcasted_iota(jnp.int32, shape, axis)


def kernel(
    pos, vel, dfm, aff, mass, vol, blk, live,
    o_d, o_v, o_f, o_c,
    pos_in, vel_in, dfm_in, aff_in, mass_in, vol_in,
    tile_a, tile_b, tile_c, coords, wx_t, wy_t, q_t, w_s, lh_s, part_s,
    select, low_s, high_s, blocks_own, blocks_got,
    top, got, from_prev, from_next,
    in_sem, top_send, top_recv, near_send, near_recv, blk_send, blk_recv,
):
    me = lax.axis_index("space")
    after = (me + 1) % 128
    before = (me + 127) % 128
    barrier = pltpu.get_barrier_semaphore()
    for offset in PEERS:
        pl.semaphore_signal(barrier, inc=1, device_id=(peer_at(me, offset),), device_id_type=MESH)

    columns = pl.ds(0, PARTICLES)
    loads = [
        pltpu.make_async_copy(vel.at[:, columns], vel_in, in_sem.at[0]),
        pltpu.make_async_copy(mass.at[pl.ds(0, TILES), :], mass_in, in_sem.at[1]),
        pltpu.make_async_copy(pos.at[:, columns], pos_in, in_sem.at[2]),
        pltpu.make_async_copy(dfm.at[:, columns], dfm_in, in_sem.at[3]),
        pltpu.make_async_copy(aff.at[:, columns], aff_in, in_sem.at[4]),
        pltpu.make_async_copy(vol.at[pl.ds(0, TILES), :], vol_in, in_sem.at[5]),
    ]
    for load in loads:
        load.start()

    alive = iota((TILES, 128), 0) // (TILES // LIVE) < live[0]
    by = [blk[b] // 16 for b in range(LIVE)]
    bz = [blk[b] % 16 for b in range(LIVE)]

    def per_bin(values, index):
        out = jnp.full(index.shape, values[LIVE - 1])
        for b in range(LIVE - 2, -1, -1):
            out = jnp.where(index == b, values[b], out)
        return out

    row_bin = iota((TILES, 128), 0) // (TILES // LIVE)
    anchor = [
        jnp.full((TILES, 128), 4 * me).astype(F32),
        (4 * per_bin(by, row_bin)).astype(F32),
        (4 * per_bin(bz, row_bin)).astype(F32),
    ]
    blocks_own[...] = per_bin([blk[b] for b in range(LIVE)], iota((8, 128), 0))

    def to_dense(source, rows, scratch, stride):
        for j in range(TILES):
            scratch[pl.ds(stride * j, rows), :] = source[:, pl.ds(128 * j, 128)]
        return [scratch[pl.ds(r, TILES, stride=stride), :] for r in range(rows)]

    loads[0].wait()
    loads[1].wait()
    v = to_dense(vel_in, 3, tile_a, 8)
    m = jnp.where(alive, mass_in[...], 0.0)

    def send_top(step, v):
        squared = jnp.where(m > 0.0, v[0] * v[0] + v[1] * v[1] + v[2] * v[2], 0.0)
        top[step] = jnp.max(squared, axis=0, keepdims=True)
        for k, offset in enumerate(PEERS):
            pltpu.make_async_remote_copy(
                top.at[step], got.at[step, k], top_send.at[step], top_recv.at[step],
                device_id=(peer_at(me, offset),), device_id_type=MESH,
            ).start()

    pl.semaphore_wait(barrier, len(PEERS))
    send_top(0, v)
    block_sends = []
    for side, target in enumerate((after, before)):
        copy = pltpu.make_async_remote_copy(
            blocks_own, blocks_got.at[side], blk_send.at[side], blk_recv.at[side],
            device_id=(target,), device_id_type=MESH,
        )
        copy.start()
        block_sends.append(copy)

    for load in loads[2:]:
        load.wait()
    x = to_dense(pos_in, 3, tile_b, 8)
    f = to_dense(dfm_in, 9, tile_c, 16)
    c = to_dense(aff_in, 9, tile_c, 16)
    volume = jnp.where(alive, vol_in[...], 0.0)
    travelled = [jnp.zeros((TILES, 128), F32)] * 3

    w_s[...] = jnp.zeros_like(w_s)
    q_t[...] = jnp.zeros_like(q_t)

    lane = iota((1, 128), 1)
    node_y = (lane % 64 // 8).astype(F32)
    node_z = (lane % 8).astype(F32)
    wide = iota((8, 512), 1)
    wide_bin = wide // 128
    node_j = 4 * per_bin(by, wide_bin) + wide % 64 // 8
    node_k = 4 * per_bin(bz, wide_bin) + wide % 8
    row = iota((8, 512), 0)
    for a in range(6):
        node_i = jnp.full((8, 512), 4 * me + a)
        lower = ((row == 0) & (node_i < 2)) | ((row == 1) & (node_j < 2)) | ((row == 2) & (node_k < 2))
        upper = ((row == 0) & (node_i >= 510)) | ((row == 1) & (node_j >= 64)) | ((row == 2) & (node_k >= 64))
        outside = (row > 2) | (node_i >= 512)
        low_s[pl.ds(8 * a, 8), :] = jnp.where(lower | outside, 0.0, -BIG)
        high_s[pl.ds(8 * a, 8), :] = jnp.where(upper | outside, 0.0, BIG)

    target_id = node_j[0:1] * 128 + node_k[0:1]

    def build_select(which, blocks_of, present):
        base = iota((64, 512), 0)
        base = base // 8 * 128 + base % 8
        for b in range(LIVE):
            block = blocks_of(b)
            source_id = base + (block // 16 * 512 + block % 16 * 4)
            same = (source_id == target_id) & present
            select[which, pl.ds(64 * b, 64), :] = jnp.where(same, 1.0, 0.0).astype(BF16)

    build_select(0, lambda b: blk[b], jnp.full((64, 512), me) >= 0)

    tile_row = iota((8, 128), 0)
    offsets = jnp.where(tile_row < 6, tile_row.astype(F32), FAR)
    left_half = lane < 64
    pair_low = tile_row < 4
    gravity = jnp.where(iota((8, 512), 0) == 0, gravity_x, jnp.where(iota((8, 512), 0) == 2, gravity_z, 0.0))
    node_y_wide = jnp.concatenate([node_y] * LIVE, axis=1)
    node_z_wide = jnp.concatenate([node_z] * LIVE, axis=1)
    left_wide = wide[0:1] % 128 < 64

    def wx_of(j, a):
        return jnp.broadcast_to(wx_t[pl.ds(8 * j + a, 1), :], (8, 128))

    near_sends = []
    for step in range(STEPS):
        local = [x[i] - anchor[i] for i in range(3)]
        for i in range(3):
            coords[i] = local[i]
        stress = kirchhoff(f)
        scaled = -4.0 * volume
        for o in range(3):
            affine_m = [m * c[3 * o + i] for i in range(3)]
            affine_s = [scaled * stress[3 * o + i] for i in range(3)]
            base_m = m * v[o]
            for i in range(3):
                base_m = base_m - affine_m[i] * local[i]
            base_s = -(affine_s[0] * local[0] + affine_s[1] * local[1] + affine_s[2] * local[2])
            q_t[0, pl.ds(o, TILES, stride=8), :] = base_m
            q_t[0, pl.ds(4 + o, TILES, stride=8), :] = base_s
            for i in range(3):
                q_t[1 + i, pl.ds(o, TILES, stride=8), :] = affine_m[i]
                q_t[1 + i, pl.ds(4 + o, TILES, stride=8), :] = affine_s[i]
        q_t[0, pl.ds(3, TILES, stride=8), :] = m

        for j in range(TILES):
            b, part = j // 4, pl.ds(128 * (j % 4), 128)
            here = pl.ds(8 * j, 8)
            near = [jnp.broadcast_to(coords[i, pl.ds(j, 1), :], (8, 128)) for i in range(3)]
            wx_t[here, :] = spline(offsets - near[0])
            wy_t[here, :] = spline(offsets - near[1])
            wz = spline(offsets - near[2])
            wyz = jnp.concatenate(
                [jnp.broadcast_to(wy_t[pl.ds(8 * j + a, 1), :], (8, 128)) * wz for a in range(6)], axis=0
            )
            high, low = halves(wyz)
            w_s[b, 0:48, part] = high
            w_s[b, 64:112, part] = high
            w_s[b, 128:176, part] = low
            w_s[b, 192:240, part] = low
            weights = [wx_of(j, a) for a in range(6)]
            q = [q_t[g, here, :] for g in range(4)]
            rows = [weights[a] * (q[0] + float(a) * q[1] if a else q[0]) for a in range(6)]
            rows += [weights[a] * q[2] for a in range(6)]
            rows += [weights[a] * q[3] for a in range(6)]
            high, low = halves(jnp.concatenate(rows, axis=0))
            lh_s[0:144, pl.ds(128 * j, 128)] = high
            lh_s[144:288, pl.ds(128 * j, 128)] = low

        totals = []
        for b in range(LIVE):
            summed = lax.dot_general(
                lh_s[:, pl.ds(PPB * b, PPB)], w_s[b], (((1,), (1,)), ((), ())), preferred_element_type=F32
            )
            totals.append(summed[0:144, 0:128] + summed[0:144, 128:256] + summed[144:288, 0:128])
        for h in range(2):
            both = jnp.where(left_half, totals[2 * h], totals[2 * h + 1])
            part_s[step, :, pl.ds(128 * h, 128)] = both[0:48] + node_y * both[48:96] + node_z * both[96:144]

        sends = [
            pltpu.make_async_remote_copy(
                part_s.at[step, pl.ds(32, 16), :], from_prev.at[step],
                near_send.at[step, 0], near_recv.at[step, 0], device_id=(after,), device_id_type=MESH,
            ),
            pltpu.make_async_remote_copy(
                part_s.at[step, pl.ds(0, 16), :], from_next.at[step],
                near_send.at[step, 1], near_recv.at[step, 1], device_id=(before,), device_id_type=MESH,
            ),
        ]
        for send in sends:
            send.start()
        near_sends += sends

        def merged(value, which):
            high, low = halves(value)
            spread = jnp.dot(
                jnp.concatenate([high, low], axis=0), select[which], preferred_element_type=F32
            )
            return spread[: value.shape[0]] + spread[value.shape[0] :]

        own = merged(part_s[step], 0)
        if step == 0:
            for copy in block_sends:
                copy.wait_recv()
            no_prev = jnp.full((64, 512), me) > 0
            no_next = jnp.full((64, 512), me) < 127
            build_select(1, lambda b: jnp.concatenate([blocks_got[0, pl.ds(b, 1), :]] * 4, axis=1), no_prev)
            build_select(2, lambda b: jnp.concatenate([blocks_got[1, pl.ds(b, 1), :]] * 4, axis=1), no_next)
        for send in sends:
            send.wait_recv()
        lower_planes = merged(from_prev[step], 1)
        upper_planes = merged(from_next[step], 2)
        planes = [own[8 * a : 8 * a + 8] for a in range(6)]
        for k in range(2):
            planes[k] = planes[k] + lower_planes[8 * k : 8 * k + 8]
            planes[4 + k] = planes[4 + k] + upper_planes[8 * k : 8 * k + 8]

        pltpu.make_async_copy(got.at[step], got.at[step], top_recv.at[step]).wait()
        fastest = jnp.maximum(top[step], jnp.max(got[step], axis=0))
        fastest = jnp.max(fastest, axis=1, keepdims=True)
        dt = courant / (jnp.sqrt(fastest) + sound_speed)

        node_rows, moments = [], []
        for a in range(6):
            here = pl.ds(8 * a, 8)
            node_mass = jnp.maximum(planes[a][3:4], mass_floor)
            momentum = planes[a] + dt * pltpu.roll(planes[a], 4, 0)
            g = momentum / node_mass + dt * gravity
            g = jnp.minimum(jnp.maximum(g, low_s[here, :]), high_s[here, :])
            node_rows.append(g + pltpu.roll(g * node_y_wide, 4, 0))
            moments.append(g * node_z_wide)
        for k in range(3):
            node_rows.append(moments[2 * k] + pltpu.roll(moments[2 * k + 1], 4, 0))
        nodes = jnp.concatenate(node_rows, axis=0)
        rounded = nodes.astype(BF16).astype(F32)
        stacked = jnp.where(left_wide, rounded, nodes - rounded).astype(BF16)

        for b in range(LIVE):
            own_nodes = stacked[:, 128 * b : 128 * b + 128]
            spread = jnp.dot(
                jnp.concatenate([own_nodes, own_nodes], axis=1), w_s[b], preferred_element_type=F32
            )
            for k in range(4):
                j = 4 * b + k
                here = pl.ds(8 * j, 8)
                t = [spread[8 * a : 8 * a + 8, 128 * k : 128 * k + 128] for a in range(9)]
                weights = [wx_of(j, a) for a in range(6)]
                terms = [weights[a] * t[a] for a in range(6)]
                plain = terms[0] + terms[1] + terms[2] + terms[3] + terms[4] + terms[5]
                first = terms[1] + 2.0 * terms[2] + 3.0 * terms[3] + 4.0 * terms[4] + 5.0 * terms[5]
                third = [
                    jnp.where(pair_low, weights[2 * h], weights[2 * h + 1]) * t[6 + h] for h in range(3)
                ]
                third = third[0] + third[1] + third[2]
                tile_a[here, :] = plain
                tile_b[here, :] = first
                tile_c[here, :] = third + pltpu.roll(third, 4, 0)

        v = [tile_a[pl.ds(o, TILES, stride=8), :] for o in range(3)]
        if step + 1 < STEPS:
            send_top(step + 1, v)
        moment = [
            [tile_b[pl.ds(o, TILES, stride=8), :] for o in range(3)],
            [tile_a[pl.ds(4 + o, TILES, stride=8), :] for o in range(3)],
            [tile_c[pl.ds(o, TILES, stride=8), :] for o in range(3)],
        ]
        c = [4.0 * (moment[i][o] - v[o] * local[i]) for o in range(3) for i in range(3)]
        f = [
            f[3 * r + s]
            + dt * (c[3 * r] * f[s] + c[3 * r + 1] * f[3 + s] + c[3 * r + 2] * f[6 + s])
            for r in range(3)
            for s in range(3)
        ]
        moved = [dt * v[i] for i in range(3)]
        x = [x[i] + moved[i] for i in range(3)]
        travelled = [travelled[i] + moved[i] for i in range(3)]

    for output, values in ((o_d, travelled), (o_v, v), (o_f, f), (o_c, c)):
        rows = len(values)
        stride = 8 if rows == 3 else 16
        scratch = tile_a if rows == 3 else tile_c
        for r in range(rows):
            scratch[pl.ds(r, TILES, stride=stride), :] = jnp.where(alive, values[r], 0.0)
        for j in range(TILES):
            output[:, pl.ds(128 * j, 128)] = scratch[pl.ds(stride * j, rows), :]
        output[:, pl.ds(PARTICLES, PARTICLES)] = jnp.zeros((rows, PARTICLES), F32)

    for send in near_sends + block_sends:
        send.wait_send()
    for step in range(STEPS):
        pltpu.make_async_copy(got.at[step], got.at[step], top_send.at[step]).wait()


def local(positions, velocity, deformation, affine, particle_mass, volume, bin_block, live_count):
    total = positions.shape[1]
    hbm = pl.BlockSpec(memory_space=pl.ANY)
    smem = pl.BlockSpec(memory_space=pltpu.SMEM)
    vmem = pl.BlockSpec(memory_space=pltpu.VMEM)
    return pl.pallas_call(
        kernel,
        out_shape=[jax.ShapeDtypeStruct((rows, total), F32) for rows in (3, 3, 9, 9)],
        in_specs=[hbm] * 6 + [smem] * 2,
        out_specs=[vmem] * 4,
        scratch_shapes=[
            pltpu.VMEM((3, PARTICLES), F32),
            pltpu.VMEM((3, PARTICLES), F32),
            pltpu.VMEM((9, PARTICLES), F32),
            pltpu.VMEM((9, PARTICLES), F32),
            pltpu.VMEM((TILES, 128), F32),
            pltpu.VMEM((TILES, 128), F32),
            pltpu.VMEM((8 * TILES, 128), F32),
            pltpu.VMEM((8 * TILES, 128), F32),
            pltpu.VMEM((16 * TILES, 128), F32),
            pltpu.VMEM((3, TILES, 128), F32),
            pltpu.VMEM((8 * TILES, 128), F32),
            pltpu.VMEM((8 * TILES, 128), F32),
            pltpu.VMEM((4, 8 * TILES, 128), F32),
            pltpu.VMEM((LIVE, 256, PPB), BF16),
            pltpu.VMEM((288, PARTICLES), BF16),
            pltpu.VMEM((STEPS, 48, 256), F32),
            pltpu.VMEM((3, 256, 512), BF16),
            pltpu.VMEM((48, 512), F32),
            pltpu.VMEM((48, 512), F32),
            pltpu.VMEM((8, 128), jnp.int32),
            pltpu.VMEM((2, 8, 128), jnp.int32),
            pltpu.VMEM((STEPS, 1, 128), F32),
            pltpu.VMEM((STEPS, len(PEERS), 1, 128), F32),
            pltpu.VMEM((STEPS, 16, 256), F32),
            pltpu.VMEM((STEPS, 16, 256), F32),
            pltpu.SemaphoreType.DMA((6,)),
            pltpu.SemaphoreType.DMA((STEPS,)),
            pltpu.SemaphoreType.DMA((STEPS,)),
            pltpu.SemaphoreType.DMA((STEPS, 2)),
            pltpu.SemaphoreType.DMA((STEPS, 2)),
            pltpu.SemaphoreType.DMA((2,)),
            pltpu.SemaphoreType.DMA((2,)),
        ],
        compiler_params=pltpu.CompilerParams(collective_id=0, has_side_effects=True),
        name="material_points",
    )(
        positions, velocity, deformation, affine,
        particle_mass.reshape(-1, 128), volume.reshape(-1, 128), bin_block, live_count,
    )


def solution(mesh):
    wide, flat = P(None, "space"), P("space")
    return jax.shard_map(
        local,
        mesh=mesh,
        in_specs=(wide,) * 4 + (flat,) * 4,
        out_specs=(wide,) * 4,
        check_vma=False,
    )
```

```python
import functools
import itertools

import jax
import jax.numpy as jnp
from jax import lax
from jax.experimental import pallas as pl
from jax.experimental.pallas import tpu as pltpu
from jax.sharding import PartitionSpec as P

STEPS = 3
LIVE = 4
PPB = 512
PARTICLES = LIVE * PPB
TILES = PARTICLES // 128
BIG = 3.4028235e38
FAR = 1e18
MESH = pl.DeviceIdType.MESH
F32 = jnp.float32
BF16 = jnp.bfloat16

mu_shear = 4.0
lame_first = 6.0
courant = 0.15
sound_speed = 3.7416573867739413
mass_floor = 0.05
gravity_x = 3.0
gravity_z = -9.0


def ring_distance(step):
    return min(step, 4 - step)


def peer_offsets():
    offsets = [o for o in itertools.product(range(4), range(4), range(4), range(2)) if any(o)]
    offsets.sort(key=lambda o: -(sum(ring_distance(c) for c in o[:3]) + 0.1 * o[3]))
    return offsets


def peer_at(me, offset):
    x, y, z, core = me // 32, me // 8 % 4, me // 2 % 4, me % 2
    x, y, z = (x + offset[0]) % 4, (y + offset[1]) % 4, (z + offset[2]) % 4
    return ((x * 4 + y) * 4 + z) * 2 + (core + offset[3]) % 2


PEERS = peer_offsets()


def halves(value):
    high = value.astype(BF16)
    return high, (value - high.astype(F32)).astype(BF16)


def spline(distance):
    magnitude = jnp.abs(distance)
    inner_part = 0.75 - magnitude * magnitude
    outer_part = 0.5 * (1.5 - magnitude) * (1.5 - magnitude)
    return jnp.where(magnitude < 0.5, inner_part, jnp.where(magnitude < 1.5, outer_part, 0.0))


def kirchhoff(f):
    determinant = (
        f[0] * (f[4] * f[8] - f[5] * f[7])
        - f[1] * (f[3] * f[8] - f[5] * f[6])
        + f[2] * (f[3] * f[7] - f[4] * f[6])
    )
    pressure = lame_first * (determinant - 1.0) * determinant
    stress = [None] * 9
    for r in range(3):
        for c in range(r, 3):
            product = f[3 * r] * f[3 * c] + f[3 * r + 1] * f[3 * c + 1] + f[3 * r + 2] * f[3 * c + 2]
            value = mu_shear * (product - 1.0) + pressure if r == c else mu_shear * product
            stress[3 * r + c] = stress[3 * c + r] = value
    return stress


def iota(shape, axis):
    return lax.broadcasted_iota(jnp.int32, shape, axis)


def kernel(
    pos, vel, dfm, aff, mass, vol, blk_hbm, live_hbm,
    o_d, o_v, o_f, o_c,
    blk, live, pos_in, vel_in, dfm_in, aff_in, mass_in, vol_in,
    tile_a, tile_b, tile_c, coords, wx_t, wy_t, q_t, w_s, lh_s, part_s,
    select, low_s, high_s, blocks_own, blocks_got,
    top, got, from_prev, from_next,
    in_sem, top_send, top_recv, near_send, near_recv, blk_send, blk_recv,
):
    me = lax.axis_index("space")
    after = (me + 1) % 128
    before = (me + 127) % 128
    barrier = pltpu.get_barrier_semaphore()
    for offset in PEERS:
        pl.semaphore_signal(barrier, inc=1, device_id=(peer_at(me, offset),), device_id_type=MESH)

    columns = pl.ds(0, PARTICLES)
    loads = [
        pltpu.make_async_copy(vel.at[:, columns], vel_in, in_sem.at[0]),
        pltpu.make_async_copy(live_hbm, live, in_sem.at[7]),
        pltpu.make_async_copy(mass.at[pl.ds(0, TILES), :], mass_in, in_sem.at[1]),
        pltpu.make_async_copy(blk_hbm, blk, in_sem.at[6]),
        pltpu.make_async_copy(pos.at[:, columns], pos_in, in_sem.at[2]),
        pltpu.make_async_copy(dfm.at[:, columns], dfm_in, in_sem.at[3]),
        pltpu.make_async_copy(aff.at[:, columns], aff_in, in_sem.at[4]),
        pltpu.make_async_copy(vol.at[pl.ds(0, TILES), :], vol_in, in_sem.at[5]),
    ]
    for load in loads:
        load.start()

    def to_dense(source, rows, scratch, stride):
        for j in range(TILES):
            scratch[pl.ds(stride * j, rows), :] = source[:, pl.ds(128 * j, 128)]
        return [scratch[pl.ds(r, TILES, stride=stride), :] for r in range(rows)]

    for load in loads[:3]:
        load.wait()
    alive = iota((TILES, 128), 0) // (TILES // LIVE) < live[0, 0]
    v = to_dense(vel_in, 3, tile_a, 8)
    m = jnp.where(alive, mass_in[...], 0.0)

    def send_top(step, v):
        squared = jnp.where(m > 0.0, v[0] * v[0] + v[1] * v[1] + v[2] * v[2], 0.0)
        top[step] = jnp.max(squared, axis=0, keepdims=True)
        for k, offset in enumerate(PEERS):
            pltpu.make_async_remote_copy(
                top.at[step], got.at[step, k], top_send.at[step], top_recv.at[step],
                device_id=(peer_at(me, offset),), device_id_type=MESH,
            ).start()

    pl.semaphore_wait(barrier, len(PEERS))
    send_top(0, v)
    loads[3].wait()
    by = [blk[b] // 16 for b in range(LIVE)]
    bz = [blk[b] % 16 for b in range(LIVE)]

    def per_bin(values, index):
        out = jnp.full(index.shape, values[LIVE - 1])
        for b in range(LIVE - 2, -1, -1):
            out = jnp.where(index == b, values[b], out)
        return out

    row_bin = iota((TILES, 128), 0) // (TILES // LIVE)
    anchor = [
        jnp.full((TILES, 128), 4 * me).astype(F32),
        (4 * per_bin(by, row_bin)).astype(F32),
        (4 * per_bin(bz, row_bin)).astype(F32),
    ]
    blocks_own[...] = per_bin([blk[b] for b in range(LIVE)], iota((8, 128), 0))

    block_sends = []
    for side, target in enumerate((after, before)):
        copy = pltpu.make_async_remote_copy(
            blocks_own, blocks_got.at[side], blk_send.at[side], blk_recv.at[side],
            device_id=(target,), device_id_type=MESH,
        )
        copy.start()
        block_sends.append(copy)

    for load in loads[4:]:
        load.wait()
    x = to_dense(pos_in, 3, tile_b, 8)
    f = to_dense(dfm_in, 9, tile_c, 16)
    c = to_dense(aff_in, 9, tile_c, 16)
    volume = jnp.where(alive, vol_in[...], 0.0)
    travelled = [jnp.zeros((TILES, 128), F32)] * 3

    w_s[...] = jnp.zeros_like(w_s)
    q_t[...] = jnp.zeros_like(q_t)

    lane = iota((1, 128), 1)
    node_y = (lane % 64 // 8).astype(F32)
    node_z = (lane % 8).astype(F32)
    wide = iota((8, 512), 1)
    wide_bin = wide // 128
    node_j = 4 * per_bin(by, wide_bin) + wide % 64 // 8
    node_k = 4 * per_bin(bz, wide_bin) + wide % 8
    row = iota((8, 512), 0)
    for a in range(6):
        node_i = jnp.full((8, 512), 4 * me + a)
        lower = ((row == 0) & (node_i < 2)) | ((row == 1) & (node_j < 2)) | ((row == 2) & (node_k < 2))
        upper = ((row == 0) & (node_i >= 510)) | ((row == 1) & (node_j >= 64)) | ((row == 2) & (node_k >= 64))
        outside = (row > 2) | (node_i >= 512)
        low_s[pl.ds(8 * a, 8), :] = jnp.where(lower | outside, 0.0, -BIG)
        high_s[pl.ds(8 * a, 8), :] = jnp.where(upper | outside, 0.0, BIG)

    target_id = node_j[0:1] * 128 + node_k[0:1]

    def build_select(which, blocks_of, present):
        base = iota((64, 512), 0)
        base = base // 8 * 128 + base % 8
        for b in range(LIVE):
            block = blocks_of(b)
            source_id = base + (block // 16 * 512 + block % 16 * 4)
            same = (source_id == target_id) & present
            select[which, pl.ds(64 * b, 64), :] = jnp.where(same, 1.0, 0.0).astype(BF16)

    build_select(0, lambda b: blk[b], jnp.full((64, 512), me) >= 0)

    tile_row = iota((8, 128), 0)
    offsets = jnp.where(tile_row < 6, tile_row.astype(F32), FAR)
    left_half = lane < 64
    pair_low = tile_row < 4
    gravity = jnp.where(iota((8, 512), 0) == 0, gravity_x, jnp.where(iota((8, 512), 0) == 2, gravity_z, 0.0))
    node_y_wide = jnp.concatenate([node_y] * LIVE, axis=1)
    node_z_wide = jnp.concatenate([node_z] * LIVE, axis=1)
    left_wide = wide[0:1] % 128 < 64

    def wx_of(j, a):
        return jnp.broadcast_to(wx_t[pl.ds(8 * j + a, 1), :], (8, 128))

    near_sends = []
    for step in range(STEPS):
        local = [x[i] - anchor[i] for i in range(3)]
        for i in range(3):
            coords[i] = local[i]
        stress = kirchhoff(f)
        scaled = -4.0 * volume
        for o in range(3):
            affine_m = [m * c[3 * o + i] for i in range(3)]
            affine_s = [scaled * stress[3 * o + i] for i in range(3)]
            base_m = m * v[o]
            for i in range(3):
                base_m = base_m - affine_m[i] * local[i]
            base_s = -(affine_s[0] * local[0] + affine_s[1] * local[1] + affine_s[2] * local[2])
            q_t[0, pl.ds(o, TILES, stride=8), :] = base_m
            q_t[0, pl.ds(4 + o, TILES, stride=8), :] = base_s
            for i in range(3):
                q_t[1 + i, pl.ds(o, TILES, stride=8), :] = affine_m[i]
                q_t[1 + i, pl.ds(4 + o, TILES, stride=8), :] = affine_s[i]
        q_t[0, pl.ds(3, TILES, stride=8), :] = m

        for j in range(TILES):
            b, part = j // 4, pl.ds(128 * (j % 4), 128)
            here = pl.ds(8 * j, 8)
            near = [jnp.broadcast_to(coords[i, pl.ds(j, 1), :], (8, 128)) for i in range(3)]
            wx_t[here, :] = spline(offsets - near[0])
            wy_t[here, :] = spline(offsets - near[1])
            wz = spline(offsets - near[2])
            wyz = jnp.concatenate(
                [jnp.broadcast_to(wy_t[pl.ds(8 * j + a, 1), :], (8, 128)) * wz for a in range(6)], axis=0
            )
            high, low = halves(wyz)
            w_s[b, 0:48, part] = high
            w_s[b, 64:112, part] = high
            w_s[b, 128:176, part] = low
            w_s[b, 192:240, part] = low
            weights = [wx_of(j, a) for a in range(6)]
            q = [q_t[g, here, :] for g in range(4)]
            rows = [weights[a] * (q[0] + float(a) * q[1] if a else q[0]) for a in range(6)]
            rows += [weights[a] * q[2] for a in range(6)]
            rows += [weights[a] * q[3] for a in range(6)]
            high, low = halves(jnp.concatenate(rows, axis=0))
            lh_s[0:144, pl.ds(128 * j, 128)] = high
            lh_s[144:288, pl.ds(128 * j, 128)] = low

        totals = []
        for b in range(LIVE):
            summed = lax.dot_general(
                lh_s[:, pl.ds(PPB * b, PPB)], w_s[b], (((1,), (1,)), ((), ())), preferred_element_type=F32
            )
            totals.append(summed[0:144, 0:128] + summed[0:144, 128:256] + summed[144:288, 0:128])
        for h in range(2):
            both = jnp.where(left_half, totals[2 * h], totals[2 * h + 1])
            part_s[step, :, pl.ds(128 * h, 128)] = both[0:48] + node_y * both[48:96] + node_z * both[96:144]

        sends = [
            pltpu.make_async_remote_copy(
                part_s.at[step, pl.ds(32, 16), :], from_prev.at[step],
                near_send.at[step, 0], near_recv.at[step, 0], device_id=(after,), device_id_type=MESH,
            ),
            pltpu.make_async_remote_copy(
                part_s.at[step, pl.ds(0, 16), :], from_next.at[step],
                near_send.at[step, 1], near_recv.at[step, 1], device_id=(before,), device_id_type=MESH,
            ),
        ]
        for send in sends:
            send.start()
        near_sends += sends

        def merged(value, which):
            high, low = halves(value)
            spread = jnp.dot(
                jnp.concatenate([high, low], axis=0), select[which], preferred_element_type=F32
            )
            return spread[: value.shape[0]] + spread[value.shape[0] :]

        own = merged(part_s[step], 0)
        if step == 0:
            for copy in block_sends:
                copy.wait_recv()
            no_prev = jnp.full((64, 512), me) > 0
            no_next = jnp.full((64, 512), me) < 127
            build_select(1, lambda b: jnp.concatenate([blocks_got[0, pl.ds(b, 1), :]] * 4, axis=1), no_prev)
            build_select(2, lambda b: jnp.concatenate([blocks_got[1, pl.ds(b, 1), :]] * 4, axis=1), no_next)
        for send in sends:
            send.wait_recv()
        lower_planes = merged(from_prev[step], 1)
        upper_planes = merged(from_next[step], 2)
        planes = [own[8 * a : 8 * a + 8] for a in range(6)]
        for k in range(2):
            planes[k] = planes[k] + lower_planes[8 * k : 8 * k + 8]
            planes[4 + k] = planes[4 + k] + upper_planes[8 * k : 8 * k + 8]

        pltpu.make_async_copy(got.at[step], got.at[step], top_recv.at[step]).wait()
        fastest = jnp.maximum(top[step], jnp.max(got[step], axis=0))
        fastest = jnp.max(fastest, axis=1, keepdims=True)
        dt = courant / (jnp.sqrt(fastest) + sound_speed)

        node_rows, moments = [], []
        for a in range(6):
            here = pl.ds(8 * a, 8)
            node_mass = jnp.maximum(planes[a][3:4], mass_floor)
            momentum = planes[a] + dt * pltpu.roll(planes[a], 4, 0)
            g = momentum / node_mass + dt * gravity
            g = jnp.minimum(jnp.maximum(g, low_s[here, :]), high_s[here, :])
            node_rows.append(g + pltpu.roll(g * node_y_wide, 4, 0))
            moments.append(g * node_z_wide)
        for k in range(3):
            node_rows.append(moments[2 * k] + pltpu.roll(moments[2 * k + 1], 4, 0))
        nodes = jnp.concatenate(node_rows, axis=0)
        rounded = nodes.astype(BF16).astype(F32)
        stacked = jnp.where(left_wide, rounded, nodes - rounded).astype(BF16)

        for b in range(LIVE):
            own_nodes = stacked[:, 128 * b : 128 * b + 128]
            spread = jnp.dot(
                jnp.concatenate([own_nodes, own_nodes], axis=1), w_s[b], preferred_element_type=F32
            )
            for k in range(4):
                j = 4 * b + k
                here = pl.ds(8 * j, 8)
                t = [spread[8 * a : 8 * a + 8, 128 * k : 128 * k + 128] for a in range(9)]
                weights = [wx_of(j, a) for a in range(6)]
                terms = [weights[a] * t[a] for a in range(6)]
                plain = terms[0] + terms[1] + terms[2] + terms[3] + terms[4] + terms[5]
                first = terms[1] + 2.0 * terms[2] + 3.0 * terms[3] + 4.0 * terms[4] + 5.0 * terms[5]
                third = [
                    jnp.where(pair_low, weights[2 * h], weights[2 * h + 1]) * t[6 + h] for h in range(3)
                ]
                third = third[0] + third[1] + third[2]
                tile_a[here, :] = plain
                tile_b[here, :] = first
                tile_c[here, :] = third + pltpu.roll(third, 4, 0)

        v = [tile_a[pl.ds(o, TILES, stride=8), :] for o in range(3)]
        if step + 1 < STEPS:
            send_top(step + 1, v)
        moment = [
            [tile_b[pl.ds(o, TILES, stride=8), :] for o in range(3)],
            [tile_a[pl.ds(4 + o, TILES, stride=8), :] for o in range(3)],
            [tile_c[pl.ds(o, TILES, stride=8), :] for o in range(3)],
        ]
        c = [4.0 * (moment[i][o] - v[o] * local[i]) for o in range(3) for i in range(3)]
        f = [
            f[3 * r + s]
            + dt * (c[3 * r] * f[s] + c[3 * r + 1] * f[3 + s] + c[3 * r + 2] * f[6 + s])
            for r in range(3)
            for s in range(3)
        ]
        moved = [dt * v[i] for i in range(3)]
        x = [x[i] + moved[i] for i in range(3)]
        travelled = [travelled[i] + moved[i] for i in range(3)]

    for output, values in ((o_d, travelled), (o_v, v), (o_f, f), (o_c, c)):
        rows = len(values)
        stride = 8 if rows == 3 else 16
        scratch = tile_a if rows == 3 else tile_c
        for r in range(rows):
            scratch[pl.ds(r, TILES, stride=stride), :] = jnp.where(alive, values[r], 0.0)
        for j in range(TILES):
            output[:, pl.ds(128 * j, 128)] = scratch[pl.ds(stride * j, rows), :]

    for send in near_sends + block_sends:
        send.wait_send()
    for step in range(STEPS):
        pltpu.make_async_copy(got.at[step], got.at[step], top_send.at[step]).wait()


def spread_out(d, v, f, c, o_d, o_v, o_f, o_c, nothing, sems):
    nothing[...] = jnp.zeros_like(nothing)
    copies = []
    for k, (source, target) in enumerate(((d, o_d), (v, o_v), (f, o_f), (c, o_c))):
        rows = source.shape[0]
        empty = nothing if rows == 9 else nothing.at[pl.ds(0, rows), :]
        copies.append(pltpu.make_async_copy(source, target.at[:, pl.ds(0, PARTICLES)], sems.at[2 * k]))
        copies.append(
            pltpu.make_async_copy(empty, target.at[:, pl.ds(PARTICLES, PARTICLES)], sems.at[2 * k + 1])
        )
    for copy in copies:
        copy.start()
    for copy in copies:
        copy.wait()


def local(positions, velocity, deformation, affine, particle_mass, volume, bin_block, live_count):
    total = positions.shape[1]
    hbm = pl.BlockSpec(memory_space=pl.ANY)
    vmem = pl.BlockSpec(memory_space=pltpu.VMEM)
    results = pl.pallas_call(
        kernel,
        out_shape=[pltpu.VMEM((rows, PARTICLES), F32) for rows in (3, 3, 9, 9)],
        in_specs=[hbm] * 8,
        out_specs=[vmem] * 4,
        scratch_shapes=[
            pltpu.SMEM((8,), jnp.int32),
            pltpu.SMEM((1, 1), jnp.int32),
            pltpu.VMEM((3, PARTICLES), F32),
            pltpu.VMEM((3, PARTICLES), F32),
            pltpu.VMEM((9, PARTICLES), F32),
            pltpu.VMEM((9, PARTICLES), F32),
            pltpu.VMEM((TILES, 128), F32),
            pltpu.VMEM((TILES, 128), F32),
            pltpu.VMEM((8 * TILES, 128), F32),
            pltpu.VMEM((8 * TILES, 128), F32),
            pltpu.VMEM((16 * TILES, 128), F32),
            pltpu.VMEM((3, TILES, 128), F32),
            pltpu.VMEM((8 * TILES, 128), F32),
            pltpu.VMEM((8 * TILES, 128), F32),
            pltpu.VMEM((4, 8 * TILES, 128), F32),
            pltpu.VMEM((LIVE, 256, PPB), BF16),
            pltpu.VMEM((288, PARTICLES), BF16),
            pltpu.VMEM((STEPS, 48, 256), F32),
            pltpu.VMEM((3, 256, 512), BF16),
            pltpu.VMEM((48, 512), F32),
            pltpu.VMEM((48, 512), F32),
            pltpu.VMEM((8, 128), jnp.int32),
            pltpu.VMEM((2, 8, 128), jnp.int32),
            pltpu.VMEM((STEPS, 1, 128), F32),
            pltpu.VMEM((STEPS, len(PEERS), 1, 128), F32),
            pltpu.VMEM((STEPS, 16, 256), F32),
            pltpu.VMEM((STEPS, 16, 256), F32),
            pltpu.SemaphoreType.DMA((8,)),
            pltpu.SemaphoreType.DMA((STEPS,)),
            pltpu.SemaphoreType.DMA((STEPS,)),
            pltpu.SemaphoreType.DMA((STEPS, 2)),
            pltpu.SemaphoreType.DMA((STEPS, 2)),
            pltpu.SemaphoreType.DMA((2,)),
            pltpu.SemaphoreType.DMA((2,)),
        ],
        compiler_params=pltpu.CompilerParams(collective_id=0, has_side_effects=True),
        name="material_points",
    )(
        positions, velocity, deformation, affine,
        particle_mass.reshape(-1, 128), volume.reshape(-1, 128), bin_block,
        live_count.reshape(1, 1),
    )
    return pl.pallas_call(
        spread_out,
        out_shape=[jax.ShapeDtypeStruct((rows, total), F32) for rows in (3, 3, 9, 9)],
        in_specs=[vmem] * 4,
        out_specs=[hbm] * 4,
        scratch_shapes=[pltpu.VMEM((9, PARTICLES), F32), pltpu.SemaphoreType.DMA((8,))],
        name="spread_out",
    )(*(pltpu.with_memory_space_constraint(result, pltpu.VMEM) for result in results))


def solution(mesh):
    wide, flat = P(None, "space"), P("space")
    return jax.shard_map(
        local,
        mesh=mesh,
        in_specs=(wide,) * 4 + (flat,) * 4,
        out_specs=(wide,) * 4,
        check_vma=False,
    )
```

```python
import functools
import itertools

import jax
import jax.numpy as jnp
from jax import lax
from jax.experimental import pallas as pl
from jax.experimental.pallas import tpu as pltpu
from jax.sharding import PartitionSpec as P

STEPS = 3
LIVE = 4
PPB = 512
PARTICLES = LIVE * PPB
TILES = PARTICLES // 128
BIG = 3.4028235e38
FAR = 1e18
MESH = pl.DeviceIdType.MESH
F32 = jnp.float32
BF16 = jnp.bfloat16

mu_shear = 4.0
lame_first = 6.0
courant = 0.15
sound_speed = 3.7416573867739413
mass_floor = 0.05
gravity_x = 3.0
gravity_z = -9.0


def ring_distance(step):
    return min(step, 4 - step)


def peer_offsets():
    offsets = [o for o in itertools.product(range(4), range(4), range(4), range(2)) if any(o)]
    offsets.sort(key=lambda o: -(sum(ring_distance(c) for c in o[:3]) + 0.1 * o[3]))
    return offsets


def peer_ids(me):
    x, y, z, core = me // 32, me // 8 % 4, me // 2 % 4, me % 2
    outer = [
        [(x + dx) % 4 * 32 + (y + dy) % 4 * 8 for dy in range(4)] for dx in range(4)
    ]
    inner = [[(z + dz) % 4 * 2 + (core + dc) % 2 for dc in range(2)] for dz in range(4)]
    return [outer[dx][dy] + inner[dz][dc] for dx, dy, dz, dc in PEERS]


PEERS = peer_offsets()


def halves(value):
    high = value.astype(BF16)
    return high, (value - high.astype(F32)).astype(BF16)


def spline(distance):
    magnitude = jnp.abs(distance)
    inner_part = 0.75 - magnitude * magnitude
    outer_part = 0.5 * (1.5 - magnitude) * (1.5 - magnitude)
    return jnp.where(magnitude < 0.5, inner_part, jnp.where(magnitude < 1.5, outer_part, 0.0))


def kirchhoff(f):
    determinant = (
        f[0] * (f[4] * f[8] - f[5] * f[7])
        - f[1] * (f[3] * f[8] - f[5] * f[6])
        + f[2] * (f[3] * f[7] - f[4] * f[6])
    )
    pressure = lame_first * (determinant - 1.0) * determinant
    stress = [None] * 9
    for r in range(3):
        for c in range(r, 3):
            product = f[3 * r] * f[3 * c] + f[3 * r + 1] * f[3 * c + 1] + f[3 * r + 2] * f[3 * c + 2]
            value = mu_shear * (product - 1.0) + pressure if r == c else mu_shear * product
            stress[3 * r + c] = stress[3 * c + r] = value
    return stress


def iota(shape, axis):
    return lax.broadcasted_iota(jnp.int32, shape, axis)


def kernel(
    pos, vel, dfm, aff, mass, vol, blk_hbm, live_hbm,
    o_d, o_v, o_f, o_c,
    blk, live, pos_in, vel_in, dfm_in, aff_in, mass_in, vol_in,
    tile_a, tile_b, tile_c, coords, wx_t, wy_t, q_t, w_s, lh_s, part_s,
    select, low_s, high_s, blocks_own, blocks_got,
    top, got, from_prev, from_next,
    in_sem, top_send, top_recv, near_send, near_recv, blk_send, blk_recv,
):
    me = lax.axis_index("space")
    after = (me + 1) % 128
    before = (me + 127) % 128
    columns = pl.ds(0, PARTICLES)
    loads = [
        pltpu.make_async_copy(vel.at[:, columns], vel_in, in_sem.at[0]),
        pltpu.make_async_copy(live_hbm, live, in_sem.at[7]),
        pltpu.make_async_copy(mass.at[pl.ds(0, TILES), :], mass_in, in_sem.at[1]),
        pltpu.make_async_copy(blk_hbm, blk, in_sem.at[6]),
        pltpu.make_async_copy(pos.at[:, columns], pos_in, in_sem.at[2]),
        pltpu.make_async_copy(dfm.at[:, columns], dfm_in, in_sem.at[3]),
        pltpu.make_async_copy(aff.at[:, columns], aff_in, in_sem.at[4]),
        pltpu.make_async_copy(vol.at[pl.ds(0, TILES), :], vol_in, in_sem.at[5]),
    ]
    for load in loads:
        load.start()

    barrier = pltpu.get_barrier_semaphore()
    peers = peer_ids(me)
    for peer in peers:
        pl.semaphore_signal(barrier, inc=1, device_id=(peer,), device_id_type=MESH)

    def to_dense(source, rows, scratch, stride):
        for j in range(TILES):
            scratch[pl.ds(stride * j, rows), :] = source[:, pl.ds(128 * j, 128)]
        return [scratch[pl.ds(r, TILES, stride=stride), :] for r in range(rows)]

    for load in loads[:3]:
        load.wait()
    alive = iota((TILES, 128), 0) // (TILES // LIVE) < live[0, 0]
    v = to_dense(vel_in, 3, tile_a, 8)
    m = jnp.where(alive, mass_in[...], 0.0)

    def find_top(step, v):
        squared = jnp.where(m > 0.0, v[0] * v[0] + v[1] * v[1] + v[2] * v[2], 0.0)
        top[step] = jnp.max(squared, axis=0, keepdims=True)

    def send_top(step):
        for k, peer in enumerate(peers):
            pltpu.make_async_remote_copy(
                top.at[step], got.at[step, k], top_send.at[step], top_recv.at[step],
                device_id=(peer,), device_id_type=MESH,
            ).start()

    pl.semaphore_wait(barrier, len(PEERS))
    find_top(0, v)
    send_top(0)
    loads[3].wait()
    by = [blk[b] // 16 for b in range(LIVE)]
    bz = [blk[b] % 16 for b in range(LIVE)]

    def per_bin(values, index):
        out = jnp.full(index.shape, values[LIVE - 1])
        for b in range(LIVE - 2, -1, -1):
            out = jnp.where(index == b, values[b], out)
        return out

    row_bin = iota((TILES, 128), 0) // (TILES // LIVE)
    anchor = [
        jnp.full((TILES, 128), 4 * me).astype(F32),
        (4 * per_bin(by, row_bin)).astype(F32),
        (4 * per_bin(bz, row_bin)).astype(F32),
    ]
    blocks_own[...] = per_bin([blk[b] for b in range(LIVE)], iota((8, 128), 0))


    def start_near(pair):
        pl.when(me < 127)(pair[0].start)
        pl.when(me > 0)(pair[1].start)

    def wait_near(pair):
        pl.when(me > 0)(pair[0].wait_recv)
        pl.when(me < 127)(pair[1].wait_recv)

    @pl.when(me == 0)
    def _():
        from_prev[...] = jnp.zeros_like(from_prev)
        blocks_got[0] = jnp.zeros_like(blocks_own)

    @pl.when(me == 127)
    def _():
        from_next[...] = jnp.zeros_like(from_next)
        blocks_got[1] = jnp.zeros_like(blocks_own)

    block_sends = []
    for side, target in enumerate((after, before)):
        copy = pltpu.make_async_remote_copy(
            blocks_own, blocks_got.at[side], blk_send.at[side], blk_recv.at[side],
            device_id=(target,), device_id_type=MESH,
        )
        block_sends.append(copy)
    start_near(block_sends)

    for load in loads[4:]:
        load.wait()
    x = to_dense(pos_in, 3, tile_b, 8)
    f = to_dense(dfm_in, 9, tile_c, 16)
    c = to_dense(aff_in, 9, tile_c, 16)
    volume = jnp.where(alive, vol_in[...], 0.0)
    travelled = [jnp.zeros((TILES, 128), F32)] * 3

    w_s[...] = jnp.zeros_like(w_s)
    q_t[...] = jnp.zeros_like(q_t)

    lane = iota((1, 128), 1)
    node_y = (lane % 64 // 8).astype(F32)
    node_z = (lane % 8).astype(F32)
    wide = iota((8, 512), 1)
    wide_bin = wide // 128
    node_j = 4 * per_bin(by, wide_bin) + wide % 64 // 8
    node_k = 4 * per_bin(bz, wide_bin) + wide % 8
    row = iota((8, 512), 0)
    for a in range(6):
        node_i = jnp.full((8, 512), 4 * me + a)
        lower = ((row == 0) & (node_i < 2)) | ((row == 1) & (node_j < 2)) | ((row == 2) & (node_k < 2))
        upper = ((row == 0) & (node_i >= 510)) | ((row == 1) & (node_j >= 64)) | ((row == 2) & (node_k >= 64))
        outside = (row > 2) | (node_i >= 512)
        low_s[pl.ds(8 * a, 8), :] = jnp.where(lower | outside, 0.0, -BIG)
        high_s[pl.ds(8 * a, 8), :] = jnp.where(upper | outside, 0.0, BIG)

    target_id = node_j[0:1] * 128 + node_k[0:1]

    def build_select(which, blocks_of, present):
        base = iota((64, 512), 0)
        base = base // 8 * 128 + base % 8
        for b in range(LIVE):
            block = blocks_of(b)
            source_id = base + (block // 16 * 512 + block % 16 * 4)
            same = (source_id == target_id) & present
            select[which, pl.ds(64 * b, 64), :] = jnp.where(same, 1.0, 0.0).astype(BF16)

    build_select(0, lambda b: blk[b], jnp.full((64, 512), me) >= 0)

    tile_row = iota((8, 128), 0)
    offsets = jnp.where(tile_row < 6, tile_row.astype(F32), FAR)
    left_half = lane < 64
    pair_low = tile_row < 4
    gravity = jnp.where(iota((8, 512), 0) == 0, gravity_x, jnp.where(iota((8, 512), 0) == 2, gravity_z, 0.0))
    node_y_wide = jnp.concatenate([node_y] * LIVE, axis=1)
    node_z_wide = jnp.concatenate([node_z] * LIVE, axis=1)
    left_wide = wide[0:1] % 128 < 64

    def wx_of(j, a):
        return jnp.broadcast_to(wx_t[pl.ds(8 * j + a, 1), :], (8, 128))

    near_sends = []
    for step in range(STEPS):
        local = [x[i] - anchor[i] for i in range(3)]
        for i in range(3):
            coords[i] = local[i]
        stress = kirchhoff(f)
        scaled = -4.0 * volume
        for o in range(3):
            affine_m = [m * c[3 * o + i] for i in range(3)]
            affine_s = [scaled * stress[3 * o + i] for i in range(3)]
            base_m = m * v[o]
            for i in range(3):
                base_m = base_m - affine_m[i] * local[i]
            base_s = -(affine_s[0] * local[0] + affine_s[1] * local[1] + affine_s[2] * local[2])
            q_t[0, pl.ds(o, TILES, stride=8), :] = base_m
            q_t[0, pl.ds(4 + o, TILES, stride=8), :] = base_s
            for i in range(3):
                q_t[1 + i, pl.ds(o, TILES, stride=8), :] = affine_m[i]
                q_t[1 + i, pl.ds(4 + o, TILES, stride=8), :] = affine_s[i]
        q_t[0, pl.ds(3, TILES, stride=8), :] = m

        for j in range(TILES):
            b, part = j // 4, pl.ds(128 * (j % 4), 128)
            here = pl.ds(8 * j, 8)
            near = [jnp.broadcast_to(coords[i, pl.ds(j, 1), :], (8, 128)) for i in range(3)]
            wx_t[here, :] = spline(offsets - near[0])
            wy_t[here, :] = spline(offsets - near[1])
            wz = spline(offsets - near[2])
            wyz = jnp.concatenate(
                [jnp.broadcast_to(wy_t[pl.ds(8 * j + a, 1), :], (8, 128)) * wz for a in range(6)], axis=0
            )
            high, low = halves(wyz)
            w_s[b, 0:48, part] = high
            w_s[b, 64:112, part] = high
            w_s[b, 128:176, part] = low
            w_s[b, 192:240, part] = low
            weights = [wx_of(j, a) for a in range(6)]
            q = [q_t[g, here, :] for g in range(4)]
            rows = [weights[a] * (q[0] + float(a) * q[1] if a else q[0]) for a in range(6)]
            rows += [weights[a] * q[2] for a in range(6)]
            rows += [weights[a] * q[3] for a in range(6)]
            high, low = halves(jnp.concatenate(rows, axis=0))
            lh_s[0:144, pl.ds(128 * j, 128)] = high
            lh_s[144:288, pl.ds(128 * j, 128)] = low

        totals = []
        for b in range(LIVE):
            summed = lax.dot_general(
                lh_s[:, pl.ds(PPB * b, PPB)], w_s[b], (((1,), (1,)), ((), ())), preferred_element_type=F32
            )
            totals.append(summed[0:144, 0:128] + summed[0:144, 128:256] + summed[144:288, 0:128])
        for h in range(2):
            both = jnp.where(left_half, totals[2 * h], totals[2 * h + 1])
            part_s[step, :, pl.ds(128 * h, 128)] = both[0:48] + node_y * both[48:96] + node_z * both[96:144]

        sends = [
            pltpu.make_async_remote_copy(
                part_s.at[step, pl.ds(32, 16), :], from_prev.at[step],
                near_send.at[step, 0], near_recv.at[step, 0], device_id=(after,), device_id_type=MESH,
            ),
            pltpu.make_async_remote_copy(
                part_s.at[step, pl.ds(0, 16), :], from_next.at[step],
                near_send.at[step, 1], near_recv.at[step, 1], device_id=(before,), device_id_type=MESH,
            ),
        ]
        start_near(sends)
        near_sends.append(sends)

        def merged(value, which):
            high, low = halves(value)
            spread = jnp.dot(
                jnp.concatenate([high, low], axis=0), select[which], preferred_element_type=F32
            )
            return spread[: value.shape[0]] + spread[value.shape[0] :]

        own = merged(part_s[step], 0)
        if step == 0:
            wait_near(block_sends)
            no_prev = jnp.full((64, 512), me) > 0
            no_next = jnp.full((64, 512), me) < 127
            build_select(1, lambda b: jnp.concatenate([blocks_got[0, pl.ds(b, 1), :]] * 4, axis=1), no_prev)
            build_select(2, lambda b: jnp.concatenate([blocks_got[1, pl.ds(b, 1), :]] * 4, axis=1), no_next)
        wait_near(sends)
        lower_planes = merged(from_prev[step], 1)
        upper_planes = merged(from_next[step], 2)
        planes = [own[8 * a : 8 * a + 8] for a in range(6)]
        for k in range(2):
            planes[k] = planes[k] + lower_planes[8 * k : 8 * k + 8]
            planes[4 + k] = planes[4 + k] + upper_planes[8 * k : 8 * k + 8]

        pltpu.make_async_copy(got.at[step], got.at[step], top_recv.at[step]).wait()
        fastest = jnp.maximum(top[step], jnp.max(got[step], axis=0))
        fastest = jnp.max(fastest, axis=1, keepdims=True)
        dt = courant / (jnp.sqrt(fastest) + sound_speed)

        node_rows, moments = [], []
        for a in range(6):
            here = pl.ds(8 * a, 8)
            node_mass = jnp.maximum(planes[a][3:4], mass_floor)
            momentum = planes[a] + dt * pltpu.roll(planes[a], 4, 0)
            g = momentum / node_mass + dt * gravity
            g = jnp.minimum(jnp.maximum(g, low_s[here, :]), high_s[here, :])
            node_rows.append(g + pltpu.roll(g * node_y_wide, 4, 0))
            moments.append(g * node_z_wide)
        for k in range(3):
            node_rows.append(moments[2 * k] + pltpu.roll(moments[2 * k + 1], 4, 0))
        nodes = jnp.concatenate(node_rows, axis=0)
        rounded = nodes.astype(BF16).astype(F32)
        stacked = jnp.where(left_wide, rounded, nodes - rounded).astype(BF16)

        for b in range(LIVE):
            own_nodes = stacked[:, 128 * b : 128 * b + 128]
            spread = jnp.dot(
                jnp.concatenate([own_nodes, own_nodes], axis=1), w_s[b], preferred_element_type=F32
            )
            for k in range(4):
                j = 4 * b + k
                here = pl.ds(8 * j, 8)
                t = [spread[8 * a : 8 * a + 8, 128 * k : 128 * k + 128] for a in range(9)]
                weights = [wx_of(j, a) for a in range(6)]
                terms = [weights[a] * t[a] for a in range(6)]
                plain = terms[0] + terms[1] + terms[2] + terms[3] + terms[4] + terms[5]
                first = terms[1] + 2.0 * terms[2] + 3.0 * terms[3] + 4.0 * terms[4] + 5.0 * terms[5]
                third = [
                    jnp.where(pair_low, weights[2 * h], weights[2 * h + 1]) * t[6 + h] for h in range(3)
                ]
                third = third[0] + third[1] + third[2]
                tile_a[here, :] = plain
                tile_b[here, :] = first
                tile_c[here, :] = third + pltpu.roll(third, 4, 0)

        v = [tile_a[pl.ds(o, TILES, stride=8), :] for o in range(3)]
        if step + 1 < STEPS:
            find_top(step + 1, v)
            send_top(step + 1)
        moment = [
            [tile_b[pl.ds(o, TILES, stride=8), :] for o in range(3)],
            [tile_a[pl.ds(4 + o, TILES, stride=8), :] for o in range(3)],
            [tile_c[pl.ds(o, TILES, stride=8), :] for o in range(3)],
        ]
        c = [4.0 * (moment[i][o] - v[o] * local[i]) for o in range(3) for i in range(3)]
        f = [
            f[3 * r + s]
            + dt * (c[3 * r] * f[s] + c[3 * r + 1] * f[3 + s] + c[3 * r + 2] * f[6 + s])
            for r in range(3)
            for s in range(3)
        ]
        moved = [dt * v[i] for i in range(3)]
        x = [x[i] + moved[i] for i in range(3)]
        travelled = [travelled[i] + moved[i] for i in range(3)]

    for output, values in ((o_d, travelled), (o_v, v), (o_f, f), (o_c, c)):
        rows = len(values)
        stride = 8 if rows == 3 else 16
        scratch = tile_a if rows == 3 else tile_c
        for r in range(rows):
            scratch[pl.ds(r, TILES, stride=stride), :] = jnp.where(alive, values[r], 0.0)
        for j in range(TILES):
            output[:, pl.ds(128 * j, 128)] = scratch[pl.ds(stride * j, rows), :]

    for pair in near_sends + [block_sends]:
        pl.when(me < 127)(pair[0].wait_send)
        pl.when(me > 0)(pair[1].wait_send)
    for step in range(STEPS):
        pltpu.make_async_copy(got.at[step], got.at[step], top_send.at[step]).wait()


def spread_out(d, v, f, c, o_d, o_v, o_f, o_c, nothing, sems):
    nothing[...] = jnp.zeros_like(nothing)
    copies = []
    for k, (source, target) in enumerate(((d, o_d), (v, o_v), (f, o_f), (c, o_c))):
        rows = source.shape[0]
        empty = nothing if rows == 9 else nothing.at[pl.ds(0, rows), :]
        copies.append(pltpu.make_async_copy(source, target.at[:, pl.ds(0, PARTICLES)], sems.at[2 * k]))
        copies.append(
            pltpu.make_async_copy(empty, target.at[:, pl.ds(PARTICLES, PARTICLES)], sems.at[2 * k + 1])
        )
    for copy in copies:
        copy.start()
    for copy in copies:
        copy.wait()


def local(positions, velocity, deformation, affine, particle_mass, volume, bin_block, live_count):
    total = positions.shape[1]
    hbm = pl.BlockSpec(memory_space=pl.ANY)
    vmem = pl.BlockSpec(memory_space=pltpu.VMEM)
    results = pl.pallas_call(
        kernel,
        out_shape=[pltpu.VMEM((rows, PARTICLES), F32) for rows in (3, 3, 9, 9)],
        in_specs=[hbm] * 8,
        out_specs=[vmem] * 4,
        scratch_shapes=[
            pltpu.SMEM((8,), jnp.int32),
            pltpu.SMEM((1, 1), jnp.int32),
            pltpu.VMEM((3, PARTICLES), F32),
            pltpu.VMEM((3, PARTICLES), F32),
            pltpu.VMEM((9, PARTICLES), F32),
            pltpu.VMEM((9, PARTICLES), F32),
            pltpu.VMEM((TILES, 128), F32),
            pltpu.VMEM((TILES, 128), F32),
            pltpu.VMEM((8 * TILES, 128), F32),
            pltpu.VMEM((8 * TILES, 128), F32),
            pltpu.VMEM((16 * TILES, 128), F32),
            pltpu.VMEM((3, TILES, 128), F32),
            pltpu.VMEM((8 * TILES, 128), F32),
            pltpu.VMEM((8 * TILES, 128), F32),
            pltpu.VMEM((4, 8 * TILES, 128), F32),
            pltpu.VMEM((LIVE, 256, PPB), BF16),
            pltpu.VMEM((288, PARTICLES), BF16),
            pltpu.VMEM((STEPS, 48, 256), F32),
            pltpu.VMEM((3, 256, 512), BF16),
            pltpu.VMEM((48, 512), F32),
            pltpu.VMEM((48, 512), F32),
            pltpu.VMEM((8, 128), jnp.int32),
            pltpu.VMEM((2, 8, 128), jnp.int32),
            pltpu.VMEM((STEPS, 1, 128), F32),
            pltpu.VMEM((STEPS, len(PEERS), 1, 128), F32),
            pltpu.VMEM((STEPS, 16, 256), F32),
            pltpu.VMEM((STEPS, 16, 256), F32),
            pltpu.SemaphoreType.DMA((8,)),
            pltpu.SemaphoreType.DMA((STEPS,)),
            pltpu.SemaphoreType.DMA((STEPS,)),
            pltpu.SemaphoreType.DMA((STEPS, 2)),
            pltpu.SemaphoreType.DMA((STEPS, 2)),
            pltpu.SemaphoreType.DMA((2,)),
            pltpu.SemaphoreType.DMA((2,)),
        ],
        compiler_params=pltpu.CompilerParams(collective_id=0, has_side_effects=True),
        name="material_points",
    )(
        positions, velocity, deformation, affine,
        particle_mass.reshape(-1, 128), volume.reshape(-1, 128), bin_block,
        live_count.reshape(1, 1),
    )
    return pl.pallas_call(
        spread_out,
        out_shape=[jax.ShapeDtypeStruct((rows, total), F32) for rows in (3, 3, 9, 9)],
        in_specs=[vmem] * 4,
        out_specs=[hbm] * 4,
        scratch_shapes=[pltpu.VMEM((9, PARTICLES), F32), pltpu.SemaphoreType.DMA((8,))],
        name="spread_out",
    )(*(pltpu.with_memory_space_constraint(result, pltpu.VMEM) for result in results))


def solution(mesh):
    wide, flat = P(None, "space"), P("space")
    return jax.shard_map(
        local,
        mesh=mesh,
        in_specs=(wide,) * 4 + (flat,) * 4,
        out_specs=(wide,) * 4,
        check_vma=False,
    )
```

```python
import functools
import itertools

import jax
import jax.numpy as jnp
from jax import lax
from jax.experimental import pallas as pl
from jax.experimental.pallas import tpu as pltpu
from jax.sharding import PartitionSpec as P

STEPS = 3
LIVE = 4
PPB = 512
PARTICLES = LIVE * PPB
TILES = PARTICLES // 128
BIG = 3.4028235e38
FAR = 1e18
MESH = pl.DeviceIdType.MESH
F32 = jnp.float32
BF16 = jnp.bfloat16

mu_shear = 4.0
lame_first = 6.0
courant = 0.15
sound_speed = 3.7416573867739413
mass_floor = 0.05
gravity_x = 3.0
gravity_z = -9.0


def ring_distance(step):
    return min(step, 4 - step)


def peer_offsets():
    offsets = [o for o in itertools.product(range(4), range(4), range(4), range(2)) if any(o)]
    offsets.sort(key=lambda o: -(sum(ring_distance(c) for c in o[:3]) + 0.1 * o[3]))
    return offsets


def peer_ids(me):
    x, y, z, core = me // 32, me // 8 % 4, me // 2 % 4, me % 2
    outer = [
        [(x + dx) % 4 * 32 + (y + dy) % 4 * 8 for dy in range(4)] for dx in range(4)
    ]
    inner = [[(z + dz) % 4 * 2 + (core + dc) % 2 for dc in range(2)] for dz in range(4)]
    return (outer[dx][dy] + inner[dz][dc] for dx, dy, dz, dc in PEERS)


PEERS = peer_offsets()
SHARED_PLANES = (0, 1, 4, 5)
INNER_PLANES = (2, 3)


def halves(value):
    high = value.astype(BF16)
    return high, (value - high.astype(F32)).astype(BF16)


def spline(distance):
    magnitude = jnp.abs(distance)
    inner_part = 0.75 - magnitude * magnitude
    outer_part = 0.5 * (1.5 - magnitude) * (1.5 - magnitude)
    return jnp.where(magnitude < 0.5, inner_part, jnp.where(magnitude < 1.5, outer_part, 0.0))


def kirchhoff(f):
    determinant = (
        f[0] * (f[4] * f[8] - f[5] * f[7])
        - f[1] * (f[3] * f[8] - f[5] * f[6])
        + f[2] * (f[3] * f[7] - f[4] * f[6])
    )
    pressure = lame_first * (determinant - 1.0) * determinant
    stress = [None] * 9
    for r in range(3):
        for c in range(r, 3):
            product = f[3 * r] * f[3 * c] + f[3 * r + 1] * f[3 * c + 1] + f[3 * r + 2] * f[3 * c + 2]
            value = mu_shear * (product - 1.0) + pressure if r == c else mu_shear * product
            stress[3 * r + c] = stress[3 * c + r] = value
    return stress


def iota(shape, axis):
    return lax.broadcasted_iota(jnp.int32, shape, axis)


def kernel(
    pos, vel, dfm, aff, mass, vol, blk_hbm, live_hbm,
    o_d, o_v, o_f, o_c,
    blk, live, pos_in, vel_in, dfm_in, aff_in, mass_in, vol_in,
    tile_a, tile_b, tile_c, coords, wx_t, wy_t, q_t, w_s, lh_s, lh_inner, part_s,
    select, low_s, high_s, blocks_own, blocks_got,
    top, got, from_prev, from_next,
    in_sem, top_send, top_recv, near_send, near_recv, blk_send, blk_recv,
):
    me = lax.axis_index("space")
    after = (me + 1) % 128
    before = (me + 127) % 128
    columns = pl.ds(0, PARTICLES)
    loads = [
        pltpu.make_async_copy(vel.at[:, columns], vel_in, in_sem.at[0]),
        pltpu.make_async_copy(live_hbm, live, in_sem.at[7]),
        pltpu.make_async_copy(mass.at[pl.ds(0, TILES), :], mass_in, in_sem.at[1]),
        pltpu.make_async_copy(blk_hbm, blk, in_sem.at[6]),
        pltpu.make_async_copy(pos.at[:, columns], pos_in, in_sem.at[2]),
        pltpu.make_async_copy(dfm.at[:, columns], dfm_in, in_sem.at[3]),
        pltpu.make_async_copy(aff.at[:, columns], aff_in, in_sem.at[4]),
        pltpu.make_async_copy(vol.at[pl.ds(0, TILES), :], vol_in, in_sem.at[5]),
    ]
    for load in loads:
        load.start()

    barrier = pltpu.get_barrier_semaphore()
    peers = []
    for peer in peer_ids(me):
        peers.append(peer)
        pl.semaphore_signal(barrier, inc=1, device_id=(peer,), device_id_type=MESH)

    def to_dense(source, rows, scratch, stride):
        for j in range(TILES):
            scratch[pl.ds(stride * j, rows), :] = source[:, pl.ds(128 * j, 128)]
        return [scratch[pl.ds(r, TILES, stride=stride), :] for r in range(rows)]

    for load in loads[:3]:
        load.wait()
    alive = iota((TILES, 128), 0) // (TILES // LIVE) < live[0, 0]
    v = to_dense(vel_in, 3, tile_a, 8)
    m = jnp.where(alive, mass_in[...], 0.0)

    def find_top(step, v):
        squared = jnp.where(m > 0.0, v[0] * v[0] + v[1] * v[1] + v[2] * v[2], 0.0)
        top[step] = jnp.max(squared, axis=0, keepdims=True)

    def send_top(step):
        for k, peer in enumerate(peers):
            pltpu.make_async_remote_copy(
                top.at[step], got.at[step, k], top_send.at[step], top_recv.at[step],
                device_id=(peer,), device_id_type=MESH,
            ).start()

    pl.semaphore_wait(barrier, len(PEERS))
    find_top(0, v)
    send_top(0)
    loads[3].wait()
    by = [blk[b] // 16 for b in range(LIVE)]
    bz = [blk[b] % 16 for b in range(LIVE)]

    def per_bin(values, index):
        out = jnp.full(index.shape, values[LIVE - 1])
        for b in range(LIVE - 2, -1, -1):
            out = jnp.where(index == b, values[b], out)
        return out

    row_bin = iota((TILES, 128), 0) // (TILES // LIVE)
    anchor = [
        jnp.full((TILES, 128), 4 * me).astype(F32),
        (4 * per_bin(by, row_bin)).astype(F32),
        (4 * per_bin(bz, row_bin)).astype(F32),
    ]
    blocks_own[...] = per_bin([blk[b] for b in range(LIVE)], iota((8, 128), 0))


    def start_near(pair):
        pl.when(me < 127)(pair[0].start)
        pl.when(me > 0)(pair[1].start)

    def wait_near(pair):
        pl.when(me > 0)(pair[0].wait_recv)
        pl.when(me < 127)(pair[1].wait_recv)

    @pl.when(me == 0)
    def _():
        from_prev[...] = jnp.zeros_like(from_prev)
        blocks_got[0] = jnp.zeros_like(blocks_own)

    @pl.when(me == 127)
    def _():
        from_next[...] = jnp.zeros_like(from_next)
        blocks_got[1] = jnp.zeros_like(blocks_own)

    block_sends = []
    for side, target in enumerate((after, before)):
        copy = pltpu.make_async_remote_copy(
            blocks_own, blocks_got.at[side], blk_send.at[side], blk_recv.at[side],
            device_id=(target,), device_id_type=MESH,
        )
        block_sends.append(copy)
    start_near(block_sends)

    for load in loads[4:]:
        load.wait()
    x = to_dense(pos_in, 3, tile_b, 8)
    f = to_dense(dfm_in, 9, tile_c, 16)
    c = to_dense(aff_in, 9, tile_c, 16)
    volume = jnp.where(alive, vol_in[...], 0.0)
    travelled = [jnp.zeros((TILES, 128), F32)] * 3

    w_s[...] = jnp.zeros_like(w_s)
    q_t[...] = jnp.zeros_like(q_t)

    lane = iota((1, 128), 1)
    node_y = (lane % 64 // 8).astype(F32)
    node_z = (lane % 8).astype(F32)
    wide = iota((8, 512), 1)
    wide_bin = wide // 128
    node_j = 4 * per_bin(by, wide_bin) + wide % 64 // 8
    node_k = 4 * per_bin(bz, wide_bin) + wide % 8
    row = iota((8, 512), 0)
    for a in range(6):
        node_i = jnp.full((8, 512), 4 * me + a)
        lower = ((row == 0) & (node_i < 2)) | ((row == 1) & (node_j < 2)) | ((row == 2) & (node_k < 2))
        upper = ((row == 0) & (node_i >= 510)) | ((row == 1) & (node_j >= 64)) | ((row == 2) & (node_k >= 64))
        outside = (row > 2) | (node_i >= 512)
        low_s[pl.ds(8 * a, 8), :] = jnp.where(lower | outside, 0.0, -BIG)
        high_s[pl.ds(8 * a, 8), :] = jnp.where(upper | outside, 0.0, BIG)

    target_id = node_j[0:1] * 128 + node_k[0:1]

    def build_select(which, blocks_of, present):
        base = iota((64, 512), 0)
        base = base // 8 * 128 + base % 8
        for b in range(LIVE):
            block = blocks_of(b)
            source_id = base + (block // 16 * 512 + block % 16 * 4)
            same = (source_id == target_id) & present
            select[which, pl.ds(64 * b, 64), :] = jnp.where(same, 1.0, 0.0).astype(BF16)

    build_select(0, lambda b: blk[b], jnp.full((64, 512), me) >= 0)

    tile_row = iota((8, 128), 0)
    offsets = jnp.where(tile_row < 6, tile_row.astype(F32), FAR)
    left_half = lane < 64
    pair_low = tile_row < 4
    gravity = jnp.where(iota((8, 512), 0) == 0, gravity_x, jnp.where(iota((8, 512), 0) == 2, gravity_z, 0.0))
    node_y_wide = jnp.concatenate([node_y] * LIVE, axis=1)
    node_z_wide = jnp.concatenate([node_z] * LIVE, axis=1)
    left_wide = wide[0:1] % 128 < 64

    def wx_of(j, a):
        return jnp.broadcast_to(wx_t[pl.ds(8 * j + a, 1), :], (8, 128))

    near_sends = []
    for step in range(STEPS):
        local = [x[i] - anchor[i] for i in range(3)]
        for i in range(3):
            coords[i] = local[i]
        stress = kirchhoff(f)
        scaled = -4.0 * volume
        for o in range(3):
            affine_m = [m * c[3 * o + i] for i in range(3)]
            affine_s = [scaled * stress[3 * o + i] for i in range(3)]
            base_m = m * v[o]
            for i in range(3):
                base_m = base_m - affine_m[i] * local[i]
            base_s = -(affine_s[0] * local[0] + affine_s[1] * local[1] + affine_s[2] * local[2])
            q_t[0, pl.ds(o, TILES, stride=8), :] = base_m
            q_t[0, pl.ds(4 + o, TILES, stride=8), :] = base_s
            for i in range(3):
                q_t[1 + i, pl.ds(o, TILES, stride=8), :] = affine_m[i]
                q_t[1 + i, pl.ds(4 + o, TILES, stride=8), :] = affine_s[i]
        q_t[0, pl.ds(3, TILES, stride=8), :] = m

        def fill(j, planes, target):
            here, count = pl.ds(8 * j, 8), 24 * len(planes)
            weights = {a: wx_of(j, a) for a in planes}
            q = [q_t[g, here, :] for g in range(4)]
            rows = [weights[a] * (q[0] + float(a) * q[1] if a else q[0]) for a in planes]
            rows += [weights[a] * q[2] for a in planes]
            rows += [weights[a] * q[3] for a in planes]
            high, low = halves(jnp.concatenate(rows, axis=0))
            target[0:count, pl.ds(128 * j, 128)] = high
            target[count : 2 * count, pl.ds(128 * j, 128)] = low

        def sum_nodes(planes, source):
            count, group = 24 * len(planes), 8 * len(planes)
            totals = []
            for b in range(LIVE):
                summed = lax.dot_general(
                    source[:, pl.ds(PPB * b, PPB)], w_s[b], (((1,), (1,)), ((), ())),
                    preferred_element_type=F32,
                )
                totals.append(
                    summed[0:count, 0:128] + summed[0:count, 128:256] + summed[count : 2 * count, 0:128]
                )
            for h in range(2):
                both = jnp.where(left_half, totals[2 * h], totals[2 * h + 1])
                both = both[0:group] + node_y * both[group : 2 * group] + node_z * both[2 * group :]
                for i, a in enumerate(planes):
                    part_s[step, pl.ds(8 * a, 8), pl.ds(128 * h, 128)] = both[8 * i : 8 * i + 8]

        for j in range(TILES):
            b, part = j // 4, pl.ds(128 * (j % 4), 128)
            here = pl.ds(8 * j, 8)
            near = [jnp.broadcast_to(coords[i, pl.ds(j, 1), :], (8, 128)) for i in range(3)]
            wx_t[here, :] = spline(offsets - near[0])
            wy_t[here, :] = spline(offsets - near[1])
            wz = spline(offsets - near[2])
            wyz = jnp.concatenate(
                [jnp.broadcast_to(wy_t[pl.ds(8 * j + a, 1), :], (8, 128)) * wz for a in range(6)], axis=0
            )
            high, low = halves(wyz)
            w_s[b, 0:48, part] = high
            w_s[b, 64:112, part] = high
            w_s[b, 128:176, part] = low
            w_s[b, 192:240, part] = low
            fill(j, SHARED_PLANES, lh_s)

        sum_nodes(SHARED_PLANES, lh_s)

        sends = [
            pltpu.make_async_remote_copy(
                part_s.at[step, pl.ds(32, 16), :], from_prev.at[step],
                near_send.at[step, 0], near_recv.at[step, 0], device_id=(after,), device_id_type=MESH,
            ),
            pltpu.make_async_remote_copy(
                part_s.at[step, pl.ds(0, 16), :], from_next.at[step],
                near_send.at[step, 1], near_recv.at[step, 1], device_id=(before,), device_id_type=MESH,
            ),
        ]
        start_near(sends)
        near_sends.append(sends)

        for j in range(TILES):
            fill(j, INNER_PLANES, lh_inner)
        sum_nodes(INNER_PLANES, lh_inner)

        def merged(value, which):
            high, low = halves(value)
            spread = jnp.dot(
                jnp.concatenate([high, low], axis=0), select[which], preferred_element_type=F32
            )
            return spread[: value.shape[0]] + spread[value.shape[0] :]

        own = merged(part_s[step], 0)
        if step == 0:
            wait_near(block_sends)
            no_prev = jnp.full((64, 512), me) > 0
            no_next = jnp.full((64, 512), me) < 127
            build_select(1, lambda b: jnp.concatenate([blocks_got[0, pl.ds(b, 1), :]] * 4, axis=1), no_prev)
            build_select(2, lambda b: jnp.concatenate([blocks_got[1, pl.ds(b, 1), :]] * 4, axis=1), no_next)
        wait_near(sends)
        lower_planes = merged(from_prev[step], 1)
        upper_planes = merged(from_next[step], 2)
        planes = [own[8 * a : 8 * a + 8] for a in range(6)]
        for k in range(2):
            planes[k] = planes[k] + lower_planes[8 * k : 8 * k + 8]
            planes[4 + k] = planes[4 + k] + upper_planes[8 * k : 8 * k + 8]

        still, driven = [], []
        for a in range(6):
            node_mass = jnp.maximum(planes[a][3:4], mass_floor)
            still.append(planes[a] / node_mass)
            driven.append(pltpu.roll(still[a], 4, 0) + gravity)

        pltpu.make_async_copy(got.at[step], got.at[step], top_recv.at[step]).wait()
        fastest = jnp.maximum(top[step], jnp.max(got[step], axis=0))
        fastest = jnp.max(fastest, axis=1, keepdims=True)
        dt = courant / (jnp.sqrt(fastest) + sound_speed)

        node_rows, moments = [], []
        for a in range(6):
            here = pl.ds(8 * a, 8)
            g = still[a] + dt * driven[a]
            g = jnp.minimum(jnp.maximum(g, low_s[here, :]), high_s[here, :])
            node_rows.append(g + pltpu.roll(g * node_y_wide, 4, 0))
            moments.append(g * node_z_wide)
        for k in range(3):
            node_rows.append(moments[2 * k] + pltpu.roll(moments[2 * k + 1], 4, 0))
        nodes = jnp.concatenate(node_rows, axis=0)
        rounded = nodes.astype(BF16).astype(F32)
        stacked = jnp.where(left_wide, rounded, nodes - rounded).astype(BF16)

        for b in range(LIVE):
            own_nodes = stacked[:, 128 * b : 128 * b + 128]
            spread = jnp.dot(
                jnp.concatenate([own_nodes, own_nodes], axis=1), w_s[b], preferred_element_type=F32
            )
            for k in range(4):
                j = 4 * b + k
                here = pl.ds(8 * j, 8)
                t = [spread[8 * a : 8 * a + 8, 128 * k : 128 * k + 128] for a in range(9)]
                weights = [wx_of(j, a) for a in range(6)]
                terms = [weights[a] * t[a] for a in range(6)]
                plain = terms[0] + terms[1] + terms[2] + terms[3] + terms[4] + terms[5]
                first = terms[1] + 2.0 * terms[2] + 3.0 * terms[3] + 4.0 * terms[4] + 5.0 * terms[5]
                third = [
                    jnp.where(pair_low, weights[2 * h], weights[2 * h + 1]) * t[6 + h] for h in range(3)
                ]
                third = third[0] + third[1] + third[2]
                tile_a[here, :] = plain
                tile_b[here, :] = first
                tile_c[here, :] = third + pltpu.roll(third, 4, 0)

        v = [tile_a[pl.ds(o, TILES, stride=8), :] for o in range(3)]
        if step + 1 < STEPS:
            find_top(step + 1, v)
            send_top(step + 1)
        moment = [
            [tile_b[pl.ds(o, TILES, stride=8), :] for o in range(3)],
            [tile_a[pl.ds(4 + o, TILES, stride=8), :] for o in range(3)],
            [tile_c[pl.ds(o, TILES, stride=8), :] for o in range(3)],
        ]
        c = [4.0 * (moment[i][o] - v[o] * local[i]) for o in range(3) for i in range(3)]
        f = [
            f[3 * r + s]
            + dt * (c[3 * r] * f[s] + c[3 * r + 1] * f[3 + s] + c[3 * r + 2] * f[6 + s])
            for r in range(3)
            for s in range(3)
        ]
        moved = [dt * v[i] for i in range(3)]
        x = [x[i] + moved[i] for i in range(3)]
        travelled = [travelled[i] + moved[i] for i in range(3)]

    for output, values in ((o_d, travelled), (o_v, v), (o_f, f), (o_c, c)):
        rows = len(values)
        stride = 8 if rows == 3 else 16
        scratch = tile_a if rows == 3 else tile_c
        for r in range(rows):
            scratch[pl.ds(r, TILES, stride=stride), :] = jnp.where(alive, values[r], 0.0)
        for j in range(TILES):
            output[:, pl.ds(128 * j, 128)] = scratch[pl.ds(stride * j, rows), :]

    for pair in near_sends + [block_sends]:
        pl.when(me < 127)(pair[0].wait_send)
        pl.when(me > 0)(pair[1].wait_send)
    for step in range(STEPS):
        pltpu.make_async_copy(got.at[step], got.at[step], top_send.at[step]).wait()


def spread_out(d, v, f, c, o_d, o_v, o_f, o_c, nothing, sems):
    nothing[...] = jnp.zeros_like(nothing)
    copies = []
    for k, (source, target) in enumerate(((d, o_d), (v, o_v), (f, o_f), (c, o_c))):
        rows = source.shape[0]
        empty = nothing if rows == 9 else nothing.at[pl.ds(0, rows), :]
        copies.append(pltpu.make_async_copy(source, target.at[:, pl.ds(0, PARTICLES)], sems.at[2 * k]))
        copies.append(
            pltpu.make_async_copy(empty, target.at[:, pl.ds(PARTICLES, PARTICLES)], sems.at[2 * k + 1])
        )
    for copy in copies:
        copy.start()
    for copy in copies:
        copy.wait()


def local(positions, velocity, deformation, affine, particle_mass, volume, bin_block, live_count):
    total = positions.shape[1]
    hbm = pl.BlockSpec(memory_space=pl.ANY)
    vmem = pl.BlockSpec(memory_space=pltpu.VMEM)
    results = pl.pallas_call(
        kernel,
        out_shape=[pltpu.VMEM((rows, PARTICLES), F32) for rows in (3, 3, 9, 9)],
        in_specs=[hbm] * 8,
        out_specs=[vmem] * 4,
        scratch_shapes=[
            pltpu.SMEM((8,), jnp.int32),
            pltpu.SMEM((1, 1), jnp.int32),
            pltpu.VMEM((3, PARTICLES), F32),
            pltpu.VMEM((3, PARTICLES), F32),
            pltpu.VMEM((9, PARTICLES), F32),
            pltpu.VMEM((9, PARTICLES), F32),
            pltpu.VMEM((TILES, 128), F32),
            pltpu.VMEM((TILES, 128), F32),
            pltpu.VMEM((8 * TILES, 128), F32),
            pltpu.VMEM((8 * TILES, 128), F32),
            pltpu.VMEM((16 * TILES, 128), F32),
            pltpu.VMEM((3, TILES, 128), F32),
            pltpu.VMEM((8 * TILES, 128), F32),
            pltpu.VMEM((8 * TILES, 128), F32),
            pltpu.VMEM((4, 8 * TILES, 128), F32),
            pltpu.VMEM((LIVE, 256, PPB), BF16),
            pltpu.VMEM((192, PARTICLES), BF16),
            pltpu.VMEM((96, PARTICLES), BF16),
            pltpu.VMEM((STEPS, 48, 256), F32),
            pltpu.VMEM((3, 256, 512), BF16),
            pltpu.VMEM((48, 512), F32),
            pltpu.VMEM((48, 512), F32),
            pltpu.VMEM((8, 128), jnp.int32),
            pltpu.VMEM((2, 8, 128), jnp.int32),
            pltpu.VMEM((STEPS, 1, 128), F32),
            pltpu.VMEM((STEPS, len(PEERS), 1, 128), F32),
            pltpu.VMEM((STEPS, 16, 256), F32),
            pltpu.VMEM((STEPS, 16, 256), F32),
            pltpu.SemaphoreType.DMA((8,)),
            pltpu.SemaphoreType.DMA((STEPS,)),
            pltpu.SemaphoreType.DMA((STEPS,)),
            pltpu.SemaphoreType.DMA((STEPS, 2)),
            pltpu.SemaphoreType.DMA((STEPS, 2)),
            pltpu.SemaphoreType.DMA((2,)),
            pltpu.SemaphoreType.DMA((2,)),
        ],
        compiler_params=pltpu.CompilerParams(collective_id=0, has_side_effects=True),
        name="material_points",
    )(
        positions, velocity, deformation, affine,
        particle_mass.reshape(-1, 128), volume.reshape(-1, 128), bin_block,
        live_count.reshape(1, 1),
    )
    return pl.pallas_call(
        spread_out,
        out_shape=[jax.ShapeDtypeStruct((rows, total), F32) for rows in (3, 3, 9, 9)],
        in_specs=[vmem] * 4,
        out_specs=[hbm] * 4,
        scratch_shapes=[pltpu.VMEM((9, PARTICLES), F32), pltpu.SemaphoreType.DMA((8,))],
        name="spread_out",
    )(*(pltpu.with_memory_space_constraint(result, pltpu.VMEM) for result in results))


def solution(mesh):
    wide, flat = P(None, "space"), P("space")
    return jax.shard_map(
        local,
        mesh=mesh,
        in_specs=(wide,) * 4 + (flat,) * 4,
        out_specs=(wide,) * 4,
        check_vma=False,
    )
```

```python
import functools
import itertools

import jax
import jax.numpy as jnp
from jax import lax
from jax.experimental import pallas as pl
from jax.experimental.pallas import tpu as pltpu
from jax.sharding import PartitionSpec as P

STEPS = 3
LIVE = 4
PPB = 512
PARTICLES = LIVE * PPB
TILES = PARTICLES // 128
BIG = 3.4028235e38
FAR = 1e18
MESH = pl.DeviceIdType.MESH
F32 = jnp.float32
BF16 = jnp.bfloat16

mu_shear = 4.0
lame_first = 6.0
courant = 0.15
sound_speed = 3.7416573867739413
mass_floor = 0.05
gravity_x = 3.0
gravity_z = -9.0


def ring_distance(step):
    return min(step, 4 - step)


def peer_offsets():
    offsets = [o for o in itertools.product(range(4), range(4), range(4), range(2)) if any(o)]
    offsets.sort(key=lambda o: -(sum(ring_distance(c) for c in o[:3]) + 0.1 * o[3]))
    return offsets


def peer_ids(me):
    x, y, z, core = me // 32, me // 8 % 4, me // 2 % 4, me % 2
    outer = [
        [(x + dx) % 4 * 32 + (y + dy) % 4 * 8 for dy in range(4)] for dx in range(4)
    ]
    inner = [[(z + dz) % 4 * 2 + (core + dc) % 2 for dc in range(2)] for dz in range(4)]
    return (outer[dx][dy] + inner[dz][dc] for dx, dy, dz, dc in PEERS)


PEERS = peer_offsets()
SHARED_PLANES = (0, 1, 4, 5)
INNER_PLANES = (2, 3)


def halves(value):
    high = value.astype(BF16)
    return high, (value - high.astype(F32)).astype(BF16)


def spline(distance):
    magnitude = jnp.abs(distance)
    inner_part = 0.75 - magnitude * magnitude
    outer_part = 0.5 * (1.5 - magnitude) * (1.5 - magnitude)
    return jnp.where(magnitude < 0.5, inner_part, jnp.where(magnitude < 1.5, outer_part, 0.0))


def kirchhoff(f):
    determinant = (
        f[0] * (f[4] * f[8] - f[5] * f[7])
        - f[1] * (f[3] * f[8] - f[5] * f[6])
        + f[2] * (f[3] * f[7] - f[4] * f[6])
    )
    pressure = lame_first * (determinant - 1.0) * determinant
    stress = [None] * 9
    for r in range(3):
        for c in range(r, 3):
            product = f[3 * r] * f[3 * c] + f[3 * r + 1] * f[3 * c + 1] + f[3 * r + 2] * f[3 * c + 2]
            value = mu_shear * (product - 1.0) + pressure if r == c else mu_shear * product
            stress[3 * r + c] = stress[3 * c + r] = value
    return stress


def iota(shape, axis):
    return lax.broadcasted_iota(jnp.int32, shape, axis)


def kernel(
    pos, vel, dfm, aff, mass, vol, blk_hbm, live_hbm,
    o_d, o_v, o_f, o_c,
    blk, live, pos_in, vel_in, dfm_in, aff_in, mass_in, vol_in,
    tile_a, tile_b, tile_c, coords, wx_t, wy_t, q_t, w_s, lh_s, lh_inner, part_s,
    select, low_s, high_s, blocks_own, blocks_got,
    top, got, from_prev, from_next,
    in_sem, top_send, top_recv, near_send, near_recv, blk_send, blk_recv,
):
    me = lax.axis_index("space")
    after = (me + 1) % 128
    before = (me + 127) % 128
    columns = pl.ds(0, PARTICLES)
    loads = [
        pltpu.make_async_copy(vel.at[:, columns], vel_in, in_sem.at[0]),
        pltpu.make_async_copy(live_hbm, live, in_sem.at[7]),
        pltpu.make_async_copy(mass.at[pl.ds(0, TILES), :], mass_in, in_sem.at[1]),
        pltpu.make_async_copy(blk_hbm, blk, in_sem.at[6]),
        pltpu.make_async_copy(pos.at[:, columns], pos_in, in_sem.at[2]),
        pltpu.make_async_copy(dfm.at[:, columns], dfm_in, in_sem.at[3]),
        pltpu.make_async_copy(aff.at[:, columns], aff_in, in_sem.at[4]),
        pltpu.make_async_copy(vol.at[pl.ds(0, TILES), :], vol_in, in_sem.at[5]),
    ]
    for load in loads:
        load.start()

    barrier = pltpu.get_barrier_semaphore()
    peers = []
    for peer in peer_ids(me):
        peers.append(peer)
        pl.semaphore_signal(barrier, inc=1, device_id=(peer,), device_id_type=MESH)

    def to_dense(source, rows, scratch, stride):
        for j in range(TILES):
            scratch[pl.ds(stride * j, rows), :] = source[:, pl.ds(128 * j, 128)]
        return [scratch[pl.ds(r, TILES, stride=stride), :] for r in range(rows)]

    for load in loads[:3]:
        load.wait()
    alive = iota((TILES, 128), 0) // (TILES // LIVE) < live[0, 0]
    v = to_dense(vel_in, 3, tile_a, 8)
    m = jnp.where(alive, mass_in[...], 0.0)

    def find_top(step, v):
        squared = jnp.where(m > 0.0, v[0] * v[0] + v[1] * v[1] + v[2] * v[2], 0.0)
        top[step] = jnp.max(squared, axis=0, keepdims=True)
        got[step, pl.ds(len(PEERS), 1), :] = top[step]

    def arrived(step):
        return got.at[step, pl.ds(0, len(PEERS)), :]

    def send_top(step):
        for k, peer in enumerate(peers):
            pltpu.make_async_remote_copy(
                top.at[step], got.at[step, pl.ds(k, 1), :], top_send.at[step], top_recv.at[step],
                device_id=(peer,), device_id_type=MESH,
            ).start()

    pl.semaphore_wait(barrier, len(PEERS))
    find_top(0, v)
    send_top(0)
    loads[3].wait()
    by = [blk[b] // 16 for b in range(LIVE)]
    bz = [blk[b] % 16 for b in range(LIVE)]

    def per_bin(values, index):
        out = jnp.full(index.shape, values[LIVE - 1])
        for b in range(LIVE - 2, -1, -1):
            out = jnp.where(index == b, values[b], out)
        return out

    row_bin = iota((TILES, 128), 0) // (TILES // LIVE)
    anchor = [
        jnp.full((TILES, 128), 4 * me).astype(F32),
        (4 * per_bin(by, row_bin)).astype(F32),
        (4 * per_bin(bz, row_bin)).astype(F32),
    ]
    blocks_own[...] = per_bin([blk[b] for b in range(LIVE)], iota((8, 128), 0))


    def start_near(pair):
        pl.when(me < 127)(pair[0].start)
        pl.when(me > 0)(pair[1].start)

    def wait_near(pair):
        pl.when(me > 0)(pair[0].wait_recv)
        pl.when(me < 127)(pair[1].wait_recv)

    @pl.when(me == 0)
    def _():
        from_prev[...] = jnp.zeros_like(from_prev)
        blocks_got[0] = jnp.zeros_like(blocks_own)

    @pl.when(me == 127)
    def _():
        from_next[...] = jnp.zeros_like(from_next)
        blocks_got[1] = jnp.zeros_like(blocks_own)

    block_sends = []
    for side, target in enumerate((after, before)):
        copy = pltpu.make_async_remote_copy(
            blocks_own, blocks_got.at[side], blk_send.at[side], blk_recv.at[side],
            device_id=(target,), device_id_type=MESH,
        )
        block_sends.append(copy)
    start_near(block_sends)

    for load in loads[4:]:
        load.wait()
    x = to_dense(pos_in, 3, tile_b, 8)
    f = to_dense(dfm_in, 9, tile_c, 16)
    c = to_dense(aff_in, 9, tile_c, 16)
    volume = jnp.where(alive, vol_in[...], 0.0)
    travelled = [jnp.zeros((TILES, 128), F32)] * 3

    w_s[...] = jnp.zeros_like(w_s)
    q_t[...] = jnp.zeros_like(q_t)

    lane = iota((1, 128), 1)
    node_y = (lane % 64 // 8).astype(F32)
    node_z = (lane % 8).astype(F32)
    wide = iota((8, 512), 1)
    wide_bin = wide // 128
    node_j = 4 * per_bin(by, wide_bin) + wide % 64 // 8
    node_k = 4 * per_bin(bz, wide_bin) + wide % 8
    row = iota((8, 512), 0)
    for a in range(6):
        node_i = jnp.full((8, 512), 4 * me + a)
        lower = ((row == 0) & (node_i < 2)) | ((row == 1) & (node_j < 2)) | ((row == 2) & (node_k < 2))
        upper = ((row == 0) & (node_i >= 510)) | ((row == 1) & (node_j >= 64)) | ((row == 2) & (node_k >= 64))
        outside = (row > 2) | (node_i >= 512)
        low_s[pl.ds(8 * a, 8), :] = jnp.where(lower | outside, 0.0, -BIG)
        high_s[pl.ds(8 * a, 8), :] = jnp.where(upper | outside, 0.0, BIG)

    target_id = node_j[0:1] * 128 + node_k[0:1]

    def build_select(which, blocks_of, present):
        base = iota((64, 512), 0)
        base = base // 8 * 128 + base % 8
        for b in range(LIVE):
            block = blocks_of(b)
            source_id = base + (block // 16 * 512 + block % 16 * 4)
            same = (source_id == target_id) & present
            select[which, pl.ds(64 * b, 64), :] = jnp.where(same, 1.0, 0.0).astype(BF16)

    build_select(0, lambda b: blk[b], jnp.full((64, 512), me) >= 0)

    tile_row = iota((8, 128), 0)
    offsets = jnp.where(tile_row < 6, tile_row.astype(F32), FAR)
    left_half = lane < 64
    pair_low = tile_row < 4
    gravity = jnp.where(iota((8, 512), 0) == 0, gravity_x, jnp.where(iota((8, 512), 0) == 2, gravity_z, 0.0))
    node_y_wide = jnp.concatenate([node_y] * LIVE, axis=1)
    node_z_wide = jnp.concatenate([node_z] * LIVE, axis=1)
    left_wide = wide[0:1] % 128 < 64

    def wx_of(j, a):
        return jnp.broadcast_to(wx_t[pl.ds(8 * j + a, 1), :], (8, 128))

    near_sends = []
    for step in range(STEPS):
        local = [x[i] - anchor[i] for i in range(3)]
        for i in range(3):
            coords[i] = local[i]
        stress = kirchhoff(f)
        scaled = -4.0 * volume
        for o in range(3):
            affine_m = [m * c[3 * o + i] for i in range(3)]
            affine_s = [scaled * stress[3 * o + i] for i in range(3)]
            base_m = m * v[o]
            for i in range(3):
                base_m = base_m - affine_m[i] * local[i]
            base_s = -(affine_s[0] * local[0] + affine_s[1] * local[1] + affine_s[2] * local[2])
            q_t[0, pl.ds(o, TILES, stride=8), :] = base_m
            q_t[0, pl.ds(4 + o, TILES, stride=8), :] = base_s
            for i in range(3):
                q_t[1 + i, pl.ds(o, TILES, stride=8), :] = affine_m[i]
                q_t[1 + i, pl.ds(4 + o, TILES, stride=8), :] = affine_s[i]
        q_t[0, pl.ds(3, TILES, stride=8), :] = m

        def fill(j, planes, target):
            here, count = pl.ds(8 * j, 8), 24 * len(planes)
            weights = {a: wx_of(j, a) for a in planes}
            q = [q_t[g, here, :] for g in range(4)]
            rows = [weights[a] * (q[0] + float(a) * q[1] if a else q[0]) for a in planes]
            rows += [weights[a] * q[2] for a in planes]
            rows += [weights[a] * q[3] for a in planes]
            high, low = halves(jnp.concatenate(rows, axis=0))
            target[0:count, pl.ds(128 * j, 128)] = high
            target[count : 2 * count, pl.ds(128 * j, 128)] = low

        def sum_nodes(planes, source):
            count, group = 24 * len(planes), 8 * len(planes)
            totals = []
            for b in range(LIVE):
                summed = lax.dot_general(
                    source[:, pl.ds(PPB * b, PPB)], w_s[b], (((1,), (1,)), ((), ())),
                    preferred_element_type=F32,
                )
                totals.append(
                    summed[0:count, 0:128] + summed[0:count, 128:256] + summed[count : 2 * count, 0:128]
                )
            for h in range(2):
                both = jnp.where(left_half, totals[2 * h], totals[2 * h + 1])
                both = both[0:group] + node_y * both[group : 2 * group] + node_z * both[2 * group :]
                for i, a in enumerate(planes):
                    part_s[step, pl.ds(8 * a, 8), pl.ds(128 * h, 128)] = both[8 * i : 8 * i + 8]

        for j in range(TILES):
            b, part = j // 4, pl.ds(128 * (j % 4), 128)
            here = pl.ds(8 * j, 8)
            near = [jnp.broadcast_to(coords[i, pl.ds(j, 1), :], (8, 128)) for i in range(3)]
            wx_t[here, :] = spline(offsets - near[0])
            wy_t[here, :] = spline(offsets - near[1])
            wz = spline(offsets - near[2])
            wyz = jnp.concatenate(
                [jnp.broadcast_to(wy_t[pl.ds(8 * j + a, 1), :], (8, 128)) * wz for a in range(6)], axis=0
            )
            high, low = halves(wyz)
            w_s[b, 0:48, part] = high
            w_s[b, 64:112, part] = high
            w_s[b, 128:176, part] = low
            w_s[b, 192:240, part] = low
            fill(j, SHARED_PLANES, lh_s)

        sum_nodes(SHARED_PLANES, lh_s)

        sends = [
            pltpu.make_async_remote_copy(
                part_s.at[step, pl.ds(32, 16), :], from_prev.at[step],
                near_send.at[step, 0], near_recv.at[step, 0], device_id=(after,), device_id_type=MESH,
            ),
            pltpu.make_async_remote_copy(
                part_s.at[step, pl.ds(0, 16), :], from_next.at[step],
                near_send.at[step, 1], near_recv.at[step, 1], device_id=(before,), device_id_type=MESH,
            ),
        ]
        start_near(sends)
        near_sends.append(sends)

        for j in range(TILES):
            fill(j, INNER_PLANES, lh_inner)
        sum_nodes(INNER_PLANES, lh_inner)

        def merged(value, which):
            high, low = halves(value)
            spread = jnp.dot(
                jnp.concatenate([high, low], axis=0), select[which], preferred_element_type=F32
            )
            return spread[: value.shape[0]] + spread[value.shape[0] :]

        own = merged(part_s[step], 0)
        if step == 0:
            wait_near(block_sends)
            no_prev = jnp.full((64, 512), me) > 0
            no_next = jnp.full((64, 512), me) < 127
            build_select(1, lambda b: jnp.concatenate([blocks_got[0, pl.ds(b, 1), :]] * 4, axis=1), no_prev)
            build_select(2, lambda b: jnp.concatenate([blocks_got[1, pl.ds(b, 1), :]] * 4, axis=1), no_next)
        wait_near(sends)
        lower_planes = merged(from_prev[step], 1)
        upper_planes = merged(from_next[step], 2)
        planes = [own[8 * a : 8 * a + 8] for a in range(6)]
        for k in range(2):
            planes[k] = planes[k] + lower_planes[8 * k : 8 * k + 8]
            planes[4 + k] = planes[4 + k] + upper_planes[8 * k : 8 * k + 8]

        still, driven = [], []
        for a in range(6):
            node_mass = jnp.maximum(planes[a][3:4], mass_floor)
            still.append(planes[a] / node_mass)
            driven.append(pltpu.roll(still[a], 4, 0) + gravity)

        pltpu.make_async_copy(arrived(step), arrived(step), top_recv.at[step]).wait()
        fastest = jnp.max(got[step], axis=0, keepdims=True)
        fastest = jnp.max(fastest, axis=1, keepdims=True)
        dt = courant / (jnp.sqrt(fastest) + sound_speed)

        node_rows, moments = [], []
        for a in range(6):
            here = pl.ds(8 * a, 8)
            g = still[a] + dt * driven[a]
            g = jnp.minimum(jnp.maximum(g, low_s[here, :]), high_s[here, :])
            node_rows.append(g + pltpu.roll(g * node_y_wide, 4, 0))
            moments.append(g * node_z_wide)
        for k in range(3):
            node_rows.append(moments[2 * k] + pltpu.roll(moments[2 * k + 1], 4, 0))
        nodes = jnp.concatenate(node_rows, axis=0)
        rounded = nodes.astype(BF16).astype(F32)
        stacked = jnp.where(left_wide, rounded, nodes - rounded).astype(BF16)

        for b in range(LIVE):
            own_nodes = stacked[:, 128 * b : 128 * b + 128]
            spread = jnp.dot(
                jnp.concatenate([own_nodes, own_nodes], axis=1), w_s[b], preferred_element_type=F32
            )
            for k in range(4):
                j = 4 * b + k
                here = pl.ds(8 * j, 8)
                t = [spread[8 * a : 8 * a + 8, 128 * k : 128 * k + 128] for a in range(9)]
                weights = [wx_of(j, a) for a in range(6)]
                terms = [weights[a] * t[a] for a in range(6)]
                plain = terms[0] + terms[1] + terms[2] + terms[3] + terms[4] + terms[5]
                first = terms[1] + 2.0 * terms[2] + 3.0 * terms[3] + 4.0 * terms[4] + 5.0 * terms[5]
                third = [
                    jnp.where(pair_low, weights[2 * h], weights[2 * h + 1]) * t[6 + h] for h in range(3)
                ]
                third = third[0] + third[1] + third[2]
                tile_a[here, :] = plain
                tile_b[here, :] = first
                tile_c[here, :] = third + pltpu.roll(third, 4, 0)

        v = [tile_a[pl.ds(o, TILES, stride=8), :] for o in range(3)]
        if step + 1 < STEPS:
            find_top(step + 1, v)
            send_top(step + 1)
        moment = [
            [tile_b[pl.ds(o, TILES, stride=8), :] for o in range(3)],
            [tile_a[pl.ds(4 + o, TILES, stride=8), :] for o in range(3)],
            [tile_c[pl.ds(o, TILES, stride=8), :] for o in range(3)],
        ]
        c = [4.0 * (moment[i][o] - v[o] * local[i]) for o in range(3) for i in range(3)]
        f = [
            f[3 * r + s]
            + dt * (c[3 * r] * f[s] + c[3 * r + 1] * f[3 + s] + c[3 * r + 2] * f[6 + s])
            for r in range(3)
            for s in range(3)
        ]
        moved = [dt * v[i] for i in range(3)]
        x = [x[i] + moved[i] for i in range(3)]
        travelled = [travelled[i] + moved[i] for i in range(3)]

    for output, values in ((o_d, travelled), (o_v, v), (o_f, f), (o_c, c)):
        rows = len(values)
        stride = 8 if rows == 3 else 16
        scratch = tile_a if rows == 3 else tile_c
        for r in range(rows):
            scratch[pl.ds(r, TILES, stride=stride), :] = jnp.where(alive, values[r], 0.0)
        for j in range(TILES):
            output[:, pl.ds(128 * j, 128)] = scratch[pl.ds(stride * j, rows), :]

    for pair in near_sends + [block_sends]:
        pl.when(me < 127)(pair[0].wait_send)
        pl.when(me > 0)(pair[1].wait_send)
    for step in range(STEPS):
        pltpu.make_async_copy(arrived(step), arrived(step), top_send.at[step]).wait()


def spread_out(d, v, f, c, o_d, o_v, o_f, o_c, nothing, sems):
    nothing[...] = jnp.zeros_like(nothing)
    copies = []
    for k, (source, target) in enumerate(((d, o_d), (v, o_v), (f, o_f), (c, o_c))):
        rows = source.shape[0]
        empty = nothing if rows == 9 else nothing.at[pl.ds(0, rows), :]
        copies.append(pltpu.make_async_copy(source, target.at[:, pl.ds(0, PARTICLES)], sems.at[2 * k]))
        copies.append(
            pltpu.make_async_copy(empty, target.at[:, pl.ds(PARTICLES, PARTICLES)], sems.at[2 * k + 1])
        )
    for copy in copies:
        copy.start()
    for copy in copies:
        copy.wait()


def local(positions, velocity, deformation, affine, particle_mass, volume, bin_block, live_count):
    total = positions.shape[1]
    hbm = pl.BlockSpec(memory_space=pl.ANY)
    vmem = pl.BlockSpec(memory_space=pltpu.VMEM)
    results = pl.pallas_call(
        kernel,
        out_shape=[pltpu.VMEM((rows, PARTICLES), F32) for rows in (3, 3, 9, 9)],
        in_specs=[hbm] * 8,
        out_specs=[vmem] * 4,
        scratch_shapes=[
            pltpu.SMEM((8,), jnp.int32),
            pltpu.SMEM((1, 1), jnp.int32),
            pltpu.VMEM((3, PARTICLES), F32),
            pltpu.VMEM((3, PARTICLES), F32),
            pltpu.VMEM((9, PARTICLES), F32),
            pltpu.VMEM((9, PARTICLES), F32),
            pltpu.VMEM((TILES, 128), F32),
            pltpu.VMEM((TILES, 128), F32),
            pltpu.VMEM((8 * TILES, 128), F32),
            pltpu.VMEM((8 * TILES, 128), F32),
            pltpu.VMEM((16 * TILES, 128), F32),
            pltpu.VMEM((3, TILES, 128), F32),
            pltpu.VMEM((8 * TILES, 128), F32),
            pltpu.VMEM((8 * TILES, 128), F32),
            pltpu.VMEM((4, 8 * TILES, 128), F32),
            pltpu.VMEM((LIVE, 256, PPB), BF16),
            pltpu.VMEM((192, PARTICLES), BF16),
            pltpu.VMEM((96, PARTICLES), BF16),
            pltpu.VMEM((STEPS, 48, 256), F32),
            pltpu.VMEM((3, 256, 512), BF16),
            pltpu.VMEM((48, 512), F32),
            pltpu.VMEM((48, 512), F32),
            pltpu.VMEM((8, 128), jnp.int32),
            pltpu.VMEM((2, 8, 128), jnp.int32),
            pltpu.VMEM((STEPS, 1, 128), F32),
            pltpu.VMEM((STEPS, len(PEERS) + 1, 128), F32),
            pltpu.VMEM((STEPS, 16, 256), F32),
            pltpu.VMEM((STEPS, 16, 256), F32),
            pltpu.SemaphoreType.DMA((8,)),
            pltpu.SemaphoreType.DMA((STEPS,)),
            pltpu.SemaphoreType.DMA((STEPS,)),
            pltpu.SemaphoreType.DMA((STEPS, 2)),
            pltpu.SemaphoreType.DMA((STEPS, 2)),
            pltpu.SemaphoreType.DMA((2,)),
            pltpu.SemaphoreType.DMA((2,)),
        ],
        compiler_params=pltpu.CompilerParams(collective_id=0, has_side_effects=True),
        name="material_points",
    )(
        positions, velocity, deformation, affine,
        particle_mass.reshape(-1, 128), volume.reshape(-1, 128), bin_block,
        live_count.reshape(1, 1),
    )
    return pl.pallas_call(
        spread_out,
        out_shape=[jax.ShapeDtypeStruct((rows, total), F32) for rows in (3, 3, 9, 9)],
        in_specs=[vmem] * 4,
        out_specs=[hbm] * 4,
        scratch_shapes=[pltpu.VMEM((9, PARTICLES), F32), pltpu.SemaphoreType.DMA((8,))],
        name="spread_out",
    )(*(pltpu.with_memory_space_constraint(result, pltpu.VMEM) for result in results))


def solution(mesh):
    wide, flat = P(None, "space"), P("space")
    return jax.shard_map(
        local,
        mesh=mesh,
        in_specs=(wide,) * 4 + (flat,) * 4,
        out_specs=(wide,) * 4,
        check_vma=False,
    )
```
